256 devices in a mesh: row: 16 (over x, y), col: 16 (over z, core).
Axes of the slice: x: 4, y: 4, z: 8, core: 2. Of those that a mesh axis runs over, the one named last changes fastest.
Arguments:
- inputs: bfloat16 [2048, 16384], P('col', 'row'), may hold values from -6 to 6
- weight: bfloat16 [16384, 16384], P('row', 'col'), may hold values from -0.046875 to 0.046875
- cotangent: bfloat16 [2048, 16384], P('row', 'col'), may hold values from -0.75 to 0.75
- scale_in: float32 [8, 16384], P(None, 'row'), may hold values from -4 to 4
- scale_out: float32 [8, 16384], P(None, 'col'), may hold values from -4 to 4
- member: int32 [2048], replicated, may hold values from 0 to 7
Outputs:
- input_grad: bfloat16 [2048, 16384], P('col', 'row')
- weight_grad: float32 [16384, 16384], P('row', 'col')
- in_factor_grad: float32 [8, 16384], P(None, 'row')
- out_factor_grad: float32 [8, 16384], P(None, 'col')
The draws below stay inside these ranges and needn't reach their ends.
All inputs are finite; a program needn't handle non-finite values.
Results may differ from the reference program's by a relative error of at most 0.0049.
Values may be sent and summed in bfloat16 or wider, within the bound.
A program may use at most 128 MiB of HBM per device.

```python
import jax
import jax.numpy as jnp

D = 16384
F = 16384
M = 8
BATCH = 2048


def place_ends(result, rng, low, high):
    spot = [jax.random.randint(jax.random.fold_in(rng, axis), (), 0, length) for axis, length in enumerate(result.shape)]
    main_axis = result.shape.index(max(result.shape))
    next_to = spot[:main_axis] + [(spot[main_axis] + 1) % result.shape[main_axis]] + spot[main_axis + 1:]
    return result.at[tuple(spot)].set(low).at[tuple(next_to)].set(high)


def shard_levels(own_key, extent, shards, low, high):
    level, own = 1.0, jax.random.fold_in(own_key, 6)
    for position, blocks in shards:
        draws = jnp.exp(jax.random.uniform(jax.random.fold_in(own, position), (blocks,), jnp.float32, low / len(shards), high / len(shards)))
        level = level * jnp.repeat(draws, extent[position] // blocks).reshape([-1 if axis == position else 1 for axis in range(len(extent))])
    return level


def scatter_about(stream_key, dims, deviation, reach, pieces=(), held_as=jnp.bfloat16):
    gain = shard_levels(stream_key, dims, pieces, -0.22, 0.18) if pieces else 1.0
    values = jax.random.normal(stream_key, dims, jnp.float32) * deviation * gain
    return jnp.minimum(jnp.maximum(values, -reach), reach).astype(held_as)


def setup_inputs(seed: int = 0) -> dict:
    streams_of = jax.random.split(jax.random.key(seed), 7)
    return {
        "inputs": scatter_about(streams_of[0], (BATCH, D), 1.0, 6.0, ((0, 16), (1, 16))),
        "weight": scatter_about(streams_of[1], (D, F), D ** -0.5, 0.046875, ((0, 16), (1, 16))),
        "cotangent": scatter_about(streams_of[2], (BATCH, F), 0.125, 0.75, ((0, 16), (1, 16))),
        "scale_in": scatter_about(streams_of[3], (M, D), 1.0, 4.0, ((1, 16),), jnp.float32),
        "scale_out": scatter_about(streams_of[4], (M, F), 1.0, 4.0, ((1, 16),), jnp.float32),
        "member": place_ends(jax.random.randint(streams_of[5], (BATCH,), 0, M), jax.random.fold_in(streams_of[5], 1), 0, M - 1).astype(jnp.int32),
    }


def reference(inputs, weight, cotangent, scale_in, scale_out, member):
    r_rows = scale_in[member]
    s_rows = scale_out[member]
    scaled_in = (inputs.astype(jnp.float32) * r_rows).astype(jnp.bfloat16)
    scaled_cot = (cotangent.astype(jnp.float32) * s_rows).astype(jnp.bfloat16)
    pre_out = jnp.dot(scaled_in, weight, preferred_element_type=jnp.float32)
    out_factor_grad = jax.ops.segment_sum(cotangent.astype(jnp.float32) * pre_out, member, num_segments=M)
    back_in = jnp.dot(scaled_cot, weight.T, preferred_element_type=jnp.float32)
    input_grad = (back_in * r_rows).astype(jnp.bfloat16)
    in_factor_grad = jax.ops.segment_sum(inputs.astype(jnp.float32) * back_in, member, num_segments=M)
    weight_grad = jnp.dot(scaled_in.T, scaled_cot, preferred_element_type=jnp.float32)
    return input_grad, weight_grad, in_factor_grad, out_factor_grad
```

```python
import jax
import jax.numpy as jnp
from jax import lax
from jax.experimental import pallas as pl
from jax.experimental.pallas import tpu as pltpu
from jax.sharding import PartitionSpec as P

MESH = pl.DeviceIdType.MESH
BF16 = jnp.bfloat16
F32 = jnp.float32
XN, YN, ZN = 4, 4, 8
ROWS = 128
HALF = 64
QUARTER = 32
BLOCKS = 16
NT = (((1,), (1,)), ((), ()))
TN = (((0,), (0,)), ((), ()))


def kernel(
    x_hbm, w_hbm, cot_hbm, sin_hbm, sout_hbm, mem_hbm,
    ig_hbm, wg_hbm, inf_hbm, outf_hbm,
    X, C, Xs, Cs, W, WT, pall, prx, sb, rb, wgs, r_own, ig_v,
    sin_v, sout_v, mem_v, sc_in, sc_out,
    acc_in, acc_in_rx, fz, fin, acc_out, fx, fy, fout,
    load_sem, store_sem,
    a_s, a_r, pa_s, pa_r, b_s, b_r, d_s, d_r, c_s, c_r,
    fp_s, fp_r, fz_s, fz_r, fh_s, fh_r, fx_s, fx_r, fy_s, fy_r,
):
    row, col = lax.axis_index("row"), lax.axis_index("col")
    x, y = lax.div(row, YN), lax.rem(row, YN)
    z, c = lax.div(col, 2), lax.rem(col, 2)
    depth, width = W.shape

    def zi(k):
        return lax.rem(z + (k % ZN), ZN)

    def at(dx, dy):
        return YN * lax.rem(x + dx, XN) + lax.rem(y + dy, YN)

    def z_dev(k):
        return (row, 2 * zi(k) + c)

    partner = (row, 2 * z + 1 - c)

    def x_dev(k):
        return (at(k % XN, 0), col)

    def y_dev(k):
        return (at(0, k % YN), col)

    def rows(block, offset=0, size=ROWS):
        return pl.ds(pl.multiple_of(block * ROWS + offset, QUARTER), size)

    def remote(src, dst, send, recv, dev):
        return pltpu.make_async_remote_copy(
            src_ref=src, dst_ref=dst, send_sem=send, recv_sem=recv,
            device_id=dev, device_id_type=MESH,
        )

    def a_copy(d, u, recv=0):
        sign = 1 - 2 * d
        block = 2 * zi(-sign * (u // 2 + recv)) + c
        half = u % 2 if d == 0 else 1 - u % 2
        part = X.at[rows(block, HALF * half, HALF)]
        return remote(part, part, a_s.at[d, u], a_r.at[d, u], z_dev(sign))

    def pa_copy(k, recv=0):
        part = X.at[rows(2 * zi(k) + ((1 - c) if recv else c))]
        return remote(part, part, pa_s.at[k], pa_r.at[k], partner)

    def b_block(h, da, db):
        da, db = da % 4, db % 4
        return at(da, db) if h == 0 else at(db, da)

    def b_dev(h, axis, sign):
        along_x = (axis == 0) == (h == 0)
        return x_dev(sign) if along_x else y_dev(sign)

    OFF = (0, -1, 1, 2)

    def b_copy(h, kind, d, s=0, recv=0):
        sign = 1 - 2 * d
        if kind == "first":
            index, block, axis, off, size = d, b_block(h, -sign * recv, 0), 0, 0, HALF
        elif kind == "first_q":
            index, block, axis = 2 + d, b_block(h, -sign * (1 + recv), 0), 0
            off, size = QUARTER * d, QUARTER
        elif kind == "second":
            index, block, axis = 4 + 2 * s + d, b_block(h, OFF[s], -sign * recv), 1
            off, size = 0, HALF
        else:
            index, block, axis = 12 + 2 * s + d, b_block(h, OFF[s], -sign * (1 + recv)), 1
            off, size = QUARTER * d, QUARTER
        part = C.at[rows(block, HALF * h + off, size)]
        return remote(part, part, b_s.at[h, index], b_r.at[h, index], b_dev(h, axis, sign))

    def d_copy(pair, recv=0):
        src = pall.at[rows(2 * pair + ((c) if recv else (1 - c)))]
        return remote(src, prx.at[rows(pair)], d_s.at[pair], d_r.at[pair], partner)

    def c_copy(d, u):
        return remote(sb.at[d, u], rb.at[d, u], c_s.at[d, u], c_r.at[d, u], z_dev(1 - 2 * d))

    both = (0, 1)

    def one_hot_t(block, copies):
        members = mem_v[pl.ds(block, 1), :]
        ids = lax.broadcasted_iota(jnp.int32, (copies, ROWS), 0)
        hit = (lax.rem(ids, 8) == members) & (ids < 24)
        return jnp.where(hit, 1.0, 0.0).astype(BF16)

    def member_rows(block, sc):
        return lax.dot_general(one_hot_t(block, 32), sc[...], TN, preferred_element_type=F32)

    def split(v, out):
        s = v[...]
        hi = s.astype(BF16).astype(F32)
        mid = (s - hi).astype(BF16).astype(F32)
        low = s - hi - mid
        out[...] = jnp.concatenate([hi, mid, low, jnp.zeros_like(s)], axis=0).astype(BF16)

    def scale_in_block(block):
        Xs[rows(block)] = (X[rows(block)].astype(F32) * member_rows(block, sc_in)).astype(BF16)

    def back_block(block):
        Cs[rows(block)] = (C[rows(block)].astype(F32) * member_rows(block, sc_out)).astype(BF16)
        lhs = Cs[rows(block)]
        for n in range(depth // 256):
            cols = pl.ds(256 * n, 256)
            pall[rows(block), cols] = jnp.dot(
                lhs, WT[:, cols], preferred_element_type=F32
            ).astype(BF16)

        @pl.when(lax.rem(block, 2) != c)
        def _():
            pair = lax.div(block, 2)
            d_copy(pair).start()

    def back_group(count, offsets):
        def body(i, carry):
            dx, dy = offsets(i)
            back_block(at(dx, dy))
            return carry
        lax.fori_loop(0, count, body, 0)

    loads = [
        pltpu.make_async_copy(x_hbm, X.at[rows(col)], load_sem.at[0]),
        pltpu.make_async_copy(cot_hbm, C.at[rows(row)], load_sem.at[1]),
        pltpu.make_async_copy(w_hbm, W, load_sem.at[2]),
        pltpu.make_async_copy(sin_hbm, sin_v, load_sem.at[3]),
        pltpu.make_async_copy(sout_hbm, sout_v, load_sem.at[4]),
        pltpu.make_async_copy(mem_hbm, mem_v, load_sem.at[5]),
    ]
    for load in loads:
        load.start()
    barrier = pltpu.get_barrier_semaphore()
    for dev in (z_dev(1), z_dev(-1), x_dev(1), x_dev(-1), y_dev(1), y_dev(-1), partner):
        pl.semaphore_signal(barrier, inc=1, device_id=dev, device_id_type=MESH)
    pl.semaphore_wait(barrier, 7)

    loads[1].wait()
    for h in both:
        for d in both:
            b_copy(h, "first", d).start()
    loads[0].wait()
    for u in (0, 1):
        for d in both:
            a_copy(d, u).start()
    for h in both:
        for d in both:
            b_copy(h, "second", d, 0).start()
    pa_copy(0).start()
    for load in loads[2:]:
        load.wait()
    split(sin_v, sc_in)
    split(sout_v, sc_out)

    def transpose_step(i, carry):
        src = pl.ds(pl.multiple_of(i * 128, 128), 128)
        for k in range(width // 256):
            WT[pl.ds(256 * k, 256), src] = W[src, pl.ds(256 * k, 256)].T
        return carry
    lax.fori_loop(0, depth // 128, transpose_step, 0)

    def a_tick(u, forward):
        for d in both:
            a_copy(d, u, 1).wait_recv()
            if forward:
                a_copy(d, u + 2).start()

    def pa_send(*ks):
        for k in ks:
            pa_copy(k).start()

    a_tick(0, True)
    for h in both:
        for d in both:
            b_copy(h, "first", d, recv=1).wait_recv()
            b_copy(h, "first_q", d).start()
    for h in both:
        for s in (1, 2):
            for d in both:
                b_copy(h, "second", d, s).start()
    back_group(1, lambda i: (0, 0))
    scale_in_block(col)

    a_tick(1, True)
    pa_send(1, 7)
    for h in both:
        for d in both:
            b_copy(h, "second", d, 0, recv=1).wait_recv()
            b_copy(h, "second_q", d, 0).start()
    back_group(2, lambda i: (1 + 2 * i, 0))

    for h in both:
        for d in both:
            b_copy(h, "first_q", d, recv=1).wait_recv()
        for d in both:
            b_copy(h, "second", d, 3).start()
    back_group(2, lambda i: (0, 1 + 2 * i))

    a_tick(2, True)
    for h in both:
        for d in both:
            b_copy(h, "second_q", d, 0, recv=1).wait_recv()
    back_group(2, lambda i: (2 - 2 * i, 2 * i))

    a_tick(3, True)
    pa_send(2, 6)

    for h in both:
        for s in (1, 2):
            for d in both:
                b_copy(h, "second", d, s, recv=1).wait_recv()
                b_copy(h, "second_q", d, s).start()
    back_group(2, lambda i: (1, 1 + 2 * i))

    a_tick(4, True)
    back_group(2, lambda i: (3, 1 + 2 * i))

    a_tick(5, False)
    pa_send(3, 5)
    for h in both:
        for d in both:
            b_copy(h, "second", d, 3, recv=1).wait_recv()
            b_copy(h, "second_q", d, 3).start()

    def scale_landed(pair):
        pa_copy(pair, 1).wait_recv()

    a_tick(6, False)
    pa_send(4)
    for h in both:
        for s in (1, 2):
            for d in both:
                b_copy(h, "second_q", d, s, recv=1).wait_recv()
    back_group(4, lambda i: (
        2 * (1 - lax.div(i, 2)) + lax.div(i, 2) * (1 + 2 * lax.rem(i, 2)),
        2 * lax.div(i, 2) + (1 - lax.div(i, 2)) * (1 + 2 * lax.rem(i, 2)),
    ))
    for h in both:
        for d in both:
            b_copy(h, "second_q", d, 3, recv=1).wait_recv()
    back_group(1, lambda i: (2, 2))

    def chip_sum(k, half=0, size=ROWS):
        pair = zi(k)
        own = pall[rows(2 * pair + c, HALF * half, size)].astype(F32)
        return own + prx[rows(pair, HALF * half, size)].astype(F32)

    def c_tick(u):
        k = 4 - (u + 1) // 2
        for d in both:
            half = u % 2 if d == 0 else 1 - u % 2
            if u >= 2:
                c_copy(d, u - 2).wait_recv()
            total = chip_sum(k if d == 0 else -k, half, HALF)
            if u >= 2:
                total += rb[d, u - 2].astype(F32)
            sb[d, u] = total.astype(BF16)
            c_copy(d, u).start()

    def d_wait(*ks):
        for k in ks:
            d_copy(zi(k), 1).wait_recv()

    def pre_piece(i, carry):
        two = pl.ds(pl.multiple_of(i * 256, 256), 256)
        lhs = Xs[two]
        hot = jnp.concatenate([one_hot_t(2 * i, 16), one_hot_t(2 * i + 1, 16)], axis=1)
        for n in range(width // 256):
            cols = pl.ds(256 * n, 256)
            pre = jnp.dot(lhs, W[:, cols], preferred_element_type=F32)
            term = (C[two, cols].astype(F32) * pre).astype(BF16)
            acc_out[:, cols] += jnp.dot(hot, term, preferred_element_type=F32)
        return carry

    def in_piece(k, carry):
        pair = lax.rem(z + k, ZN)
        block = 2 * pair + c
        hot = one_hot_t(block, 16)
        for n in range(depth // 256):
            cols = pl.ds(256 * n, 256)
            total = pall[rows(block), cols].astype(F32) + prx[rows(pair), cols].astype(F32)
            term = (X[rows(block), cols].astype(F32) * total).astype(BF16)
            acc_in[:, cols] += jnp.dot(hot, term, preferred_element_type=F32)
        return carry

    def wg_piece(i):
        cols = pl.ds(256 * i, 256)
        for n in range(width // 256):
            wgs[cols, pl.ds(256 * n, 256)] = lax.dot_general(
                Xs[:, cols], Cs[:, pl.ds(256 * n, 256)], TN, preferred_element_type=F32
            )
        pltpu.make_async_copy(wgs.at[cols], wg_hbm.at[cols], store_sem.at[i]).start()

    acc_in[...] = jnp.zeros_like(acc_in)
    acc_out[...] = jnp.zeros_like(acc_out)
    d_wait(4, 3, 5)
    c_tick(0)
    c_tick(1)
    for k in range(ZN):
        pa_copy(k, 1).wait_recv()

    def scale_step(i, carry):
        scale_in_block(i)
        return carry
    d_wait(2, 6, 1, 7, 0)
    lax.fori_loop(0, BLOCKS, scale_step, 0)
    c_tick(2)
    lax.fori_loop(0, ZN, in_piece, 0)
    in_swap = remote(acc_in, acc_in_rx, fp_s.at[0], fp_r.at[0], partner)
    in_swap.start()
    lax.fori_loop(0, 2, pre_piece, 0)
    c_tick(3)
    in_swap.wait_recv()

    my_half = pl.ds(pl.multiple_of(c * (depth // 2), depth // 2), depth // 2)
    other_half = pl.ds(pl.multiple_of((1 - c) * (depth // 2), depth // 2), depth // 2)
    fz[z] = acc_in[:8, my_half] + acc_in_rx[:8, my_half]

    def fz_copy(d, u, recv=0):
        sign = 1 - 2 * d
        slot = fz.at[zi(-sign * (u + recv))]
        return remote(slot, slot, fz_s.at[d, u], fz_r.at[d, u], z_dev(sign))

    fz_copy(0, 0).start()
    fz_copy(1, 0).start()
    lax.fori_loop(2, 5, pre_piece, 0)
    c_tick(4)
    for d in both:
        fz_copy(d, 0, 1).wait_recv()
        fz_copy(d, 1).start()
    lax.fori_loop(5, 8, pre_piece, 0)

    def fx_copy(i, recv=0):
        sign = -1 if i == 1 else 1
        slot = fx.at[lax.rem(x + ((-sign * recv - (i == 2)) % XN), XN)]
        return remote(slot, slot, fx_s.at[i], fx_r.at[i], x_dev(sign))

    def fy_copy(i, recv=0):
        sign = -1 if i == 1 else 1
        slot = fy.at[lax.rem(y + ((-sign * recv - (i == 2)) % YN), YN)]
        return remote(slot, slot, fy_s.at[i], fy_r.at[i], y_dev(sign))

    fx[x] = acc_out[:8, :]
    fx_copy(0).start()
    fx_copy(1).start()
    c_tick(5)
    for d in both:
        fz_copy(d, 1, 1).wait_recv()
        fz_copy(d, 2).start()
    wg_piece(0)
    fx_copy(0, 1).wait_recv()
    fx_copy(2).start()
    wg_piece(1)
    c_tick(6)
    for d in both:
        fz_copy(d, 2, 1).wait_recv()
    fz_copy(0, 3).start()
    fx_copy(1, 1).wait_recv()
    fx_copy(2, 1).wait_recv()
    fy[y] = ((fx[0] + fx[1]) + fx[2]) + fx[3]
    fy_copy(0).start()
    fy_copy(1).start()
    wg_piece(2)
    fy_copy(0, 1).wait_recv()
    fy_copy(2).start()
    wg_piece(3)
    r_own[...] = member_rows(col, sc_in)

    fz_copy(0, 3, 1).wait_recv()
    total_in = fz[0]
    for k in range(1, ZN):
        total_in += fz[k]
    fin[:, my_half] = total_in
    half_swap = remote(fin.at[:, my_half], fin.at[:, my_half], fh_s.at[0], fh_r.at[0], partner)
    half_swap.start()
    half_back = remote(fin.at[:, other_half], fin.at[:, other_half], fh_s.at[0], fh_r.at[0], partner)

    fy_copy(1, 1).wait_recv()
    fy_copy(2, 1).wait_recv()
    fout[...] = ((fy[0] + fy[1]) + fy[2]) + fy[3]
    store_out = pltpu.make_async_copy(fout, outf_hbm, store_sem.at[4])
    store_out.start()
    half_back.wait_recv()
    store_in = pltpu.make_async_copy(fin, inf_hbm, store_sem.at[5])
    store_in.start()

    for d in both:
        c_copy(d, 5).wait_recv()
    for d in both:
        c_copy(d, 6).wait_recv()
    for half in both:
        part = pl.ds(HALF * half, HALF)
        total = chip_sum(0, half, HALF)
        total += rb[0, 6 - half].astype(F32) + rb[1, 5 + half].astype(F32)
        ig_v[part] = (total * r_own[part]).astype(BF16)
    store_ig = pltpu.make_async_copy(ig_v, ig_hbm, store_sem.at[6])
    store_ig.start()

    for d in both:
        for u in range(7):
            a_copy(d, u).wait_send()
            c_copy(d, u).wait_send()
    for k in range(ZN):
        pa_copy(k).wait_send()
        d_copy(k).wait_send()
    for h in both:
        for d in both:
            b_copy(h, "first", d).wait_send()
            b_copy(h, "first_q", d).wait_send()
            for s in range(4):
                b_copy(h, "second", d, s).wait_send()
                b_copy(h, "second_q", d, s).wait_send()
    in_swap.wait_send()
    half_swap.wait_send()
    for u in range(3):
        fx_copy(u).wait_send()
        fy_copy(u).wait_send()
        for d in both:
            fz_copy(d, u).wait_send()
    fz_copy(0, 3).wait_send()
    for i in range(4):
        cols = pl.ds(256 * i, 256)
        pltpu.make_async_copy(wgs.at[cols], wg_hbm.at[cols], store_sem.at[i]).wait()
    store_out.wait()
    store_in.wait()
    store_ig.wait()


def local(inputs, weight, cotangent, scale_in, scale_out, member):
    depth, width = weight.shape
    batch = BLOCKS * ROWS
    anywhere = pl.BlockSpec(memory_space=pl.ANY)
    dma = pltpu.SemaphoreType.DMA
    return pl.pallas_call(
        kernel,
        out_shape=(
            jax.ShapeDtypeStruct((ROWS, depth), BF16),
            jax.ShapeDtypeStruct((depth, width), F32),
            jax.ShapeDtypeStruct((8, depth), F32),
            jax.ShapeDtypeStruct((8, width), F32),
        ),
        in_specs=[anywhere] * 6,
        out_specs=(anywhere,) * 4,
        scratch_shapes=[
            pltpu.VMEM((batch, depth), BF16),
            pltpu.VMEM((batch, width), BF16),
            pltpu.VMEM((batch, depth), BF16),
            pltpu.VMEM((batch, width), BF16),
            pltpu.VMEM((depth, width), BF16),
            pltpu.VMEM((width, depth), BF16),
            pltpu.VMEM((batch, depth), BF16),
            pltpu.VMEM((batch // 2, depth), BF16),
            pltpu.VMEM((2, 7, HALF, depth), BF16),
            pltpu.VMEM((2, 7, HALF, depth), BF16),
            pltpu.VMEM((depth, width), F32),
            pltpu.VMEM((ROWS, depth), F32),
            pltpu.VMEM((ROWS, depth), BF16),
            pltpu.VMEM((8, depth), F32),
            pltpu.VMEM((8, width), F32),
            pltpu.VMEM((BLOCKS, ROWS), jnp.int32),
            pltpu.VMEM((32, depth), BF16),
            pltpu.VMEM((32, width), BF16),
            pltpu.VMEM((16, depth), F32),
            pltpu.VMEM((16, depth), F32),
            pltpu.VMEM((ZN, 8, depth // 2), F32),
            pltpu.VMEM((8, depth), F32),
            pltpu.VMEM((16, width), F32),
            pltpu.VMEM((XN, 8, width), F32),
            pltpu.VMEM((YN, 8, width), F32),
            pltpu.VMEM((8, width), F32),
            dma((6,)), dma((7,)),
            dma((2, 7)), dma((2, 7)), dma((8,)), dma((8,)),
            dma((2, 20)), dma((2, 20)), dma((8,)), dma((8,)),
            dma((2, 7)), dma((2, 7)),
            dma((1,)), dma((1,)), dma((2, 4)), dma((2, 4)),
            dma((1,)), dma((1,)), dma((3,)), dma((3,)), dma((3,)), dma((3,)),
        ],
        compiler_params=pltpu.CompilerParams(
            collective_id=0, has_side_effects=True, vmem_limit_bytes=60 * 1024 * 1024
        ),
    )(inputs, weight, cotangent, scale_in, scale_out, member.reshape(BLOCKS, ROWS))


def solution(mesh):
    placed = (
        P("col", "row"),
        P("row", "col"),
        P("row", "col"),
        P(None, "row"),
        P(None, "col"),
        P(),
    )
    return jax.shard_map(
        local,
        mesh=mesh,
        in_specs=placed,
        out_specs=(P("col", "row"), P("row", "col"), P(None, "row"), P(None, "col")),
        check_vma=False,
    )
```

```python
import jax
import jax.numpy as jnp
from jax import lax
from jax.experimental import pallas as pl
from jax.experimental.pallas import tpu as pltpu
from jax.sharding import PartitionSpec as P

MESH = pl.DeviceIdType.MESH
BF16 = jnp.bfloat16
F32 = jnp.float32
XN, YN, ZN = 4, 4, 8
ROWS = 128
HALF = 64
QUARTER = 32
BLOCKS = 16
TN = (((0,), (0,)), ((), ()))


def kernel(
    x_hbm, w_hbm, cot_hbm, sin_hbm, sout_hbm, mem_hbm,
    ig_v, wgs, fin, fout,
    X, C, Xs, Cs, W, WT, pall, prx, sb, rb, r_own,
    sin_v, sout_v, mem_v, sc_in, sc_out,
    hot, hot_c, terms, in_terms, acc_in, acc_in_rx, fz, fx, fy,
    load_sem,
    a_s, a_r, pa_s, pa_r, b_s, b_r, d_s, d_r, c_s, c_r,
    fp_s, fp_r, fz_s, fz_r, fh_s, fh_r, fx_s, fx_r, fy_s, fy_r,
):
    row, col = lax.axis_index("row"), lax.axis_index("col")
    x, y = lax.div(row, YN), lax.rem(row, YN)
    z, c = lax.div(col, 2), lax.rem(col, 2)
    depth, width = W.shape

    def zi(k):
        return lax.rem(z + (k % ZN), ZN)

    def at(dx, dy):
        return YN * lax.rem(x + dx, XN) + lax.rem(y + dy, YN)

    def z_dev(k):
        return (row, 2 * zi(k) + c)

    partner = (row, 2 * z + 1 - c)

    def x_dev(k):
        return (at(k % XN, 0), col)

    def y_dev(k):
        return (at(0, k % YN), col)

    def rows(block, offset=0, size=ROWS):
        return pl.ds(pl.multiple_of(block * ROWS + offset, QUARTER), size)

    def lanes(block):
        return pl.ds(pl.multiple_of(block * ROWS, ROWS), ROWS)

    def remote(src, dst, send, recv, dev):
        return pltpu.make_async_remote_copy(
            src_ref=src, dst_ref=dst, send_sem=send, recv_sem=recv,
            device_id=dev, device_id_type=MESH,
        )

    def a_copy(d, u, recv=0):
        sign = 1 - 2 * d
        block = 2 * zi(-sign * (u // 2 + recv)) + c
        half = u % 2 if d == 0 else 1 - u % 2
        part = X.at[rows(block, HALF * half, HALF)]
        return remote(part, part, a_s.at[d, u], a_r.at[d, u], z_dev(sign))

    def pa_copy(k, recv=0):
        part = X.at[rows(2 * zi(k) + ((1 - c) if recv else c))]
        return remote(part, part, pa_s.at[k], pa_r.at[k], partner)

    def b_block(h, da, db):
        da, db = da % 4, db % 4
        return at(da, db) if h == 0 else at(db, da)

    def b_dev(h, axis, sign):
        along_x = (axis == 0) == (h == 0)
        return x_dev(sign) if along_x else y_dev(sign)

    OFF = (0, -1, 1, 2)

    def b_copy(h, kind, d, s=0, recv=0):
        sign = 1 - 2 * d
        if kind == "first":
            index, block, axis, off, size = d, b_block(h, -sign * recv, 0), 0, 0, HALF
        elif kind == "first_q":
            index, block, axis = 2 + d, b_block(h, -sign * (1 + recv), 0), 0
            off, size = QUARTER * d, QUARTER
        elif kind == "second":
            index, block, axis = 4 + 2 * s + d, b_block(h, OFF[s], -sign * recv), 1
            off, size = 0, HALF
        else:
            index, block, axis = 12 + 2 * s + d, b_block(h, OFF[s], -sign * (1 + recv)), 1
            off, size = QUARTER * d, QUARTER
        part = C.at[rows(block, HALF * h + off, size)]
        return remote(part, part, b_s.at[h, index], b_r.at[h, index], b_dev(h, axis, sign))

    def d_copy(pair, recv=0):
        src = pall.at[rows(2 * pair + ((c) if recv else (1 - c)))]
        return remote(src, prx.at[rows(pair)], d_s.at[pair], d_r.at[pair], partner)

    def c_copy(d, u):
        return remote(sb.at[d, u], rb.at[d, u], c_s.at[d, u], c_r.at[d, u], z_dev(1 - 2 * d))

    both = (0, 1)

    def make_hot(i, carry):
        members = mem_v[pl.ds(i, 1), :]
        ids = lax.broadcasted_iota(jnp.int32, (32, ROWS), 0)
        hit = (lax.rem(ids, 8) == members) & (ids < 24)
        hot[:, lanes(i)] = jnp.where(hit, 1.0, 0.0).astype(BF16)
        return carry

    def member_rows(blocks, sc):
        ones = [hot[:, lanes(block)] for block in blocks]
        ones = ones[0] if len(ones) == 1 else jnp.concatenate(ones, axis=1)
        return lax.dot_general(ones, sc[...], TN, preferred_element_type=F32)

    def split(v, out):
        s = v[...]
        hi = s.astype(BF16).astype(F32)
        mid = (s - hi).astype(BF16).astype(F32)
        low = s - hi - mid
        out[...] = jnp.concatenate([hi, mid, low, jnp.zeros_like(s)], axis=0).astype(BF16)

    def scale(blocks, src, sc, dst):
        factor = member_rows(blocks, sc)
        for i, block in enumerate(blocks):
            part = factor[ROWS * i : ROWS * (i + 1)]
            dst[rows(block)] = (src[rows(block)].astype(F32) * part).astype(BF16)

    def back_blocks(*places):
        blocks = [at(dx, dy) for dx, dy in places]
        scale(blocks, C, sc_out, Cs)
        lhs = [Cs[rows(block)] for block in blocks]
        lhs = lhs[0] if len(lhs) == 1 else jnp.concatenate(lhs, axis=0)
        for n in range(depth // 256):
            cols = pl.ds(256 * n, 256)
            product = jnp.dot(lhs, WT[:, cols], preferred_element_type=F32).astype(BF16)
            for i, block in enumerate(blocks):
                pall[rows(block), cols] = product[ROWS * i : ROWS * (i + 1)]
        for block in blocks:
            @pl.when(lax.rem(block, 2) != c)
            def _():
                d_copy(lax.div(block, 2)).start()

    def pre_pair(k, landed):
        pair = zi(k)
        scale([2 * pair, 2 * pair + 1], X, sc_in, Xs)
        two = rows(2 * pair, 0, 2 * ROWS)
        lhs = Xs[two]
        for n in range(width // 256):
            cols = pl.ds(256 * n, 256)
            pre = jnp.dot(lhs, W[:, cols], preferred_element_type=F32)
            if landed:
                pre = C[two, cols].astype(F32) * pre
            terms[two, cols] = pre.astype(BF16)

    loads = [
        pltpu.make_async_copy(x_hbm, X.at[rows(col)], load_sem.at[0]),
        pltpu.make_async_copy(cot_hbm, C.at[rows(row)], load_sem.at[1]),
        pltpu.make_async_copy(w_hbm, W, load_sem.at[2]),
        pltpu.make_async_copy(sin_hbm, sin_v, load_sem.at[3]),
        pltpu.make_async_copy(sout_hbm, sout_v, load_sem.at[4]),
        pltpu.make_async_copy(mem_hbm, mem_v, load_sem.at[5]),
    ]
    for load in loads:
        load.start()
    barrier = pltpu.get_barrier_semaphore()
    for dev in (z_dev(1), z_dev(-1), x_dev(1), x_dev(-1), y_dev(1), y_dev(-1), partner):
        pl.semaphore_signal(barrier, inc=1, device_id=dev, device_id_type=MESH)
    pl.semaphore_wait(barrier, 7)

    loads[1].wait()
    for h in both:
        for d in both:
            b_copy(h, "first", d).start()
    loads[0].wait()
    for u in (0, 1):
        for d in both:
            a_copy(d, u).start()
    for h in both:
        for d in both:
            b_copy(h, "second", d, 0).start()
    pa_copy(0).start()
    for load in loads[2:]:
        load.wait()
    split(sin_v, sc_in)
    split(sout_v, sc_out)
    lax.fori_loop(0, BLOCKS, make_hot, 0)

    def transpose_step(i, carry):
        src = pl.ds(pl.multiple_of(i * 128, 128), 128)
        for k in range(width // 256):
            WT[pl.ds(256 * k, 256), src] = W[src, pl.ds(256 * k, 256)].T
        return carry
    lax.fori_loop(0, depth // 128, transpose_step, 0)
    back_blocks((0, 0))

    def a_tick(u, forward=True):
        for d in both:
            a_copy(d, u, 1).wait_recv()
            if forward:
                a_copy(d, u + 2).start()

    def pa_send(*ks):
        for k in ks:
            pa_copy(k).start()

    def pa_wait(*ks):
        for k in ks:
            pa_copy(k, 1).wait_recv()

    def b_wait(kind, s=0):
        for h in both:
            for d in both:
                b_copy(h, kind, d, s, recv=1).wait_recv()

    a_tick(0)
    for h in both:
        for d in both:
            b_copy(h, "first", d, recv=1).wait_recv()
            b_copy(h, "first_q", d).start()
    for h in both:
        for s in (1, 2):
            for d in both:
                b_copy(h, "second", d, s).start()
    a_tick(1)
    pa_send(1, 7)
    for h in both:
        for d in both:
            b_copy(h, "second", d, 0, recv=1).wait_recv()
            b_copy(h, "second_q", d, 0).start()
    back_blocks((1, 0), (3, 0))

    for h in both:
        for d in both:
            b_copy(h, "first_q", d, recv=1).wait_recv()
        for d in both:
            b_copy(h, "second", d, 3).start()
    back_blocks((0, 1), (0, 3))

    a_tick(2)
    pa_wait(0)
    pre_pair(0, False)
    pa_wait(1)
    pre_pair(1, False)
    a_tick(3)
    pa_send(2, 6)
    for h in both:
        for s in (1, 2):
            for d in both:
                b_copy(h, "second", d, s, recv=1).wait_recv()
                b_copy(h, "second_q", d, s).start()
    back_blocks((1, 1), (1, 3))
    a_tick(4)
    b_wait("second_q", 0)
    back_blocks((2, 0), (0, 2))
    back_blocks((3, 1), (3, 3))

    a_tick(5, False)
    pa_send(3, 5)
    for h in both:
        for d in both:
            b_copy(h, "second", d, 3, recv=1).wait_recv()
            b_copy(h, "second_q", d, 3).start()
    pa_wait(7)
    pre_pair(-1, False)
    pa_wait(2)
    pre_pair(2, False)

    a_tick(6, False)
    pa_send(4)
    b_wait("second_q", 1)
    b_wait("second_q", 2)
    back_blocks((2, 1), (2, 3))
    back_blocks((1, 2), (3, 2))
    b_wait("second_q", 3)
    back_blocks((2, 2))

    def chip_sum(k, half=0, size=ROWS):
        pair = zi(k)
        own = pall[rows(2 * pair + c, HALF * half, size)].astype(F32)
        return own + prx[rows(pair, HALF * half, size)].astype(F32)

    def c_tick(u, relay=None):
        k = 4 - (u + 1) // 2
        for d in both:
            half = u % 2 if d == 0 else 1 - u % 2
            if u >= 2:
                c_copy(d, u - 2).wait_recv()
            total = chip_sum(k if d == 0 else -k, half, HALF)
            if u >= 2:
                total += rb[d, u - 2].astype(F32)
            sb[d, u] = total.astype(BF16)
            if relay is not None:
                relay(d)
            c_copy(d, u).start()

    def d_wait(*ks):
        for k in ks:
            d_copy(zi(k), 1).wait_recv()

    def in_piece(pair, carry):
        block = 2 * pair + c
        total = pall[rows(block)].astype(F32) + prx[rows(pair)].astype(F32)
        in_terms[rows(pair)] = (X[rows(block)].astype(F32) * total).astype(BF16)
        hot_c[:, lanes(pair)] = hot[:16, lanes(block)]
        return carry

    def wg_piece(i):
        cols = pl.ds(256 * i, 256)
        for n in range(width // 256):
            wgs[cols, pl.ds(256 * n, 256)] = lax.dot_general(
                Xs[:, cols], Cs[:, pl.ds(256 * n, 256)], TN, preferred_element_type=F32
            )

    my_half = pl.ds(pl.multiple_of(c * (depth // 2), depth // 2), depth // 2)
    other_half = pl.ds(pl.multiple_of((1 - c) * (depth // 2), depth // 2), depth // 2)
    in_swap = remote(acc_in, acc_in_rx, fp_s.at[0], fp_r.at[0], partner)
    half_swap = remote(fin.at[:, my_half], fin.at[:, my_half], fh_s.at[0], fh_r.at[0], partner)
    half_back = remote(fin.at[:, other_half], fin.at[:, other_half], fh_s.at[0], fh_r.at[0], partner)

    def fz_copy(d, u, recv=0):
        sign = 1 - 2 * d
        slot = fz.at[zi(-sign * (u + recv))]
        return remote(slot, slot, fz_s.at[d, u], fz_r.at[d, u], z_dev(sign))

    def fz_hop(u):
        def relay(d):
            if u > 0:
                fz_copy(d, u - 1, 1).wait_recv()
            if u < 3 or d == 0:
                fz_copy(d, u).start()
        return relay

    def fx_copy(i, recv=0):
        sign = -1 if i == 1 else 1
        slot = fx.at[lax.rem(x + ((-sign * recv - (i == 2)) % XN), XN)]
        return remote(slot, slot, fx_s.at[i], fx_r.at[i], x_dev(sign))

    def fy_copy(i, recv=0):
        sign = -1 if i == 1 else 1
        slot = fy.at[lax.rem(y + ((-sign * recv - (i == 2)) % YN), YN)]
        return remote(slot, slot, fy_s.at[i], fy_r.at[i], y_dev(sign))

    d_wait(4, 3, 5)
    c_tick(0)
    c_tick(1)
    d_wait(2, 6, 1, 7, 0)
    lax.fori_loop(0, ZN, in_piece, 0)
    acc_in[...] = jnp.dot(hot_c[...], in_terms[...], preferred_element_type=F32)[:8]
    in_swap.start()
    pa_wait(6)
    pre_pair(-2, True)
    pa_wait(3)
    pre_pair(3, True)
    in_swap.wait_recv()
    fz[z] = acc_in[:, my_half] + acc_in_rx[:, my_half]
    c_tick(2, fz_hop(0))
    pa_wait(4, 5)
    pre_pair(-3, True)
    pre_pair(4, True)

    def late_term(i, carry):
        two = rows(2 * lax.rem(z + i + ZN - 1, ZN), 0, 2 * ROWS)
        terms[two] = (C[two].astype(F32) * terms[two].astype(F32)).astype(BF16)
        return carry
    lax.fori_loop(0, 4, late_term, 0)
    c_tick(3, fz_hop(1))
    fx[x] = jnp.dot(hot[:16], terms[...], preferred_element_type=F32)[:8]
    fx_copy(0).start()
    fx_copy(1).start()
    wg_piece(0)
    c_tick(4, fz_hop(2))
    fx_copy(0, 1).wait_recv()
    fx_copy(2).start()
    wg_piece(1)
    fx_copy(1, 1).wait_recv()
    fx_copy(2, 1).wait_recv()
    fy[y] = ((fx[0] + fx[1]) + fx[2]) + fx[3]
    fy_copy(0).start()
    fy_copy(1).start()
    c_tick(5, fz_hop(3))
    wg_piece(2)
    fy_copy(0, 1).wait_recv()
    fy_copy(2).start()
    c_tick(6)
    r_own[...] = member_rows([col], sc_in)
    wg_piece(3)
    fz_copy(0, 3, 1).wait_recv()
    total_in = fz[0]
    for k in range(1, ZN):
        total_in += fz[k]
    fin[:, my_half] = total_in
    half_swap.start()
    fy_copy(1, 1).wait_recv()
    fy_copy(2, 1).wait_recv()
    fout[...] = ((fy[0] + fy[1]) + fy[2]) + fy[3]
    half_back.wait_recv()

    for d in both:
        c_copy(d, 5).wait_recv()
    for d in both:
        c_copy(d, 6).wait_recv()
    for half in both:
        part = pl.ds(HALF * half, HALF)
        total = chip_sum(0, half, HALF)
        total += rb[0, 6 - half].astype(F32) + rb[1, 5 + half].astype(F32)
        ig_v[part] = (total * r_own[part]).astype(BF16)

    for d in both:
        for u in range(7):
            a_copy(d, u).wait_send()
            c_copy(d, u).wait_send()
    for k in range(ZN):
        pa_copy(k).wait_send()
        d_copy(k).wait_send()
    for h in both:
        for d in both:
            b_copy(h, "first", d).wait_send()
            b_copy(h, "first_q", d).wait_send()
            for s in range(4):
                b_copy(h, "second", d, s).wait_send()
                b_copy(h, "second_q", d, s).wait_send()
    in_swap.wait_send()
    half_swap.wait_send()
    for u in range(3):
        fx_copy(u).wait_send()
        fy_copy(u).wait_send()
        for d in both:
            fz_copy(d, u).wait_send()
    fz_copy(0, 3).wait_send()


def local(inputs, weight, cotangent, scale_in, scale_out, member):
    depth, width = weight.shape
    batch = BLOCKS * ROWS
    in_hbm = pl.BlockSpec(memory_space=pltpu.HBM)
    dma = pltpu.SemaphoreType.DMA
    return pl.pallas_call(
        kernel,
        out_shape=(
            pltpu.VMEM((ROWS, depth), BF16),
            pltpu.VMEM((depth, width), F32),
            pltpu.VMEM((8, depth), F32),
            pltpu.VMEM((8, width), F32),
        ),
        in_specs=[in_hbm] * 6,
        out_specs=(pl.BlockSpec(memory_space=pltpu.VMEM),) * 4,
        scratch_shapes=[
            pltpu.VMEM((batch, depth), BF16),
            pltpu.VMEM((batch, width), BF16),
            pltpu.VMEM((batch, depth), BF16),
            pltpu.VMEM((batch, width), BF16),
            pltpu.VMEM((depth, width), BF16),
            pltpu.VMEM((width, depth), BF16),
            pltpu.VMEM((batch, depth), BF16),
            pltpu.VMEM((batch // 2, depth), BF16),
            pltpu.VMEM((2, 7, HALF, depth), BF16),
            pltpu.VMEM((2, 7, HALF, depth), BF16),
            pltpu.VMEM((ROWS, depth), F32),
            pltpu.VMEM((8, depth), F32),
            pltpu.VMEM((8, width), F32),
            pltpu.VMEM((BLOCKS, ROWS), jnp.int32),
            pltpu.VMEM((32, depth), BF16),
            pltpu.VMEM((32, width), BF16),
            pltpu.VMEM((32, batch), BF16),
            pltpu.VMEM((16, batch // 2), BF16),
            pltpu.VMEM((batch, width), BF16),
            pltpu.VMEM((batch // 2, depth), BF16),
            pltpu.VMEM((8, depth), F32),
            pltpu.VMEM((8, depth), F32),
            pltpu.VMEM((ZN, 8, depth // 2), F32),
            pltpu.VMEM((XN, 8, width), F32),
            pltpu.VMEM((YN, 8, width), F32),
            dma((6,)),
            dma((2, 7)), dma((2, 7)), dma((8,)), dma((8,)),
            dma((2, 20)), dma((2, 20)), dma((8,)), dma((8,)),
            dma((2, 7)), dma((2, 7)),
            dma((1,)), dma((1,)), dma((2, 4)), dma((2, 4)),
            dma((1,)), dma((1,)), dma((3,)), dma((3,)), dma((3,)), dma((3,)),
        ],
        compiler_params=pltpu.CompilerParams(
            collective_id=0, has_side_effects=True, vmem_limit_bytes=62500000
        ),
    )(inputs, weight, cotangent, scale_in, scale_out, member.reshape(BLOCKS, ROWS))


def solution(mesh):
    placed = (
        P("col", "row"),
        P("row", "col"),
        P("row", "col"),
        P(None, "row"),
        P(None, "col"),
        P(),
    )
    return jax.shard_map(
        local,
        mesh=mesh,
        in_specs=placed,
        out_specs=(P("col", "row"), P("row", "col"), P(None, "row"), P(None, "col")),
        check_vma=False,
    )
```

```python
import jax
import jax.numpy as jnp
from jax import lax
from jax.experimental import pallas as pl
from jax.experimental.pallas import tpu as pltpu
from jax.sharding import PartitionSpec as P

MESH = pl.DeviceIdType.MESH
BF16 = jnp.bfloat16
F32 = jnp.float32
XN, YN, ZN = 4, 4, 8
ROWS = 128
HALF = 64
PHASES = 2
STEP = 32
BLOCKS = 16
TN = (((0,), (0,)), ((), ()))


def kernel(
    x_hbm, w_hbm, cot_hbm, sin_hbm, sout_hbm, mem_hbm,
    ig_v, wgs, fin, fout,
    X, C, Xs, Cs, W, WT, pall, prx, sb, rb, r_own,
    sin_v, sout_v, mem_v, sc_in, sc_out,
    hot, hot_rows, terms, in_terms, swap_out, swap_in, fz, fx, fy,
    load_sem,
    a_s, a_r, pa_s, pa_r, b_s, b_r, d_s, d_r, c_s, c_r,
    fp_s, fp_r, fz_s, fz_r, fx_s, fx_r, fy_s, fy_r,
):
    row, col = lax.axis_index("row"), lax.axis_index("col")
    x, y = lax.div(row, YN), lax.rem(row, YN)
    z, c = lax.div(col, 2), lax.rem(col, 2)
    depth, width = W.shape
    both = (0, 1)
    hd = [(h, d) for h in both for d in both]

    def zi(k):
        return lax.rem(z + (k % ZN), ZN)

    def at(dx, dy):
        return YN * lax.rem(x + dx, XN) + lax.rem(y + dy, YN)

    def z_dev(k):
        return (row, 2 * zi(k) + c)

    partner = (row, 2 * z + 1 - c)

    def x_dev(k):
        return (at(k % XN, 0), col)

    def y_dev(k):
        return (at(0, k % YN), col)

    def rows(block, offset=0, size=ROWS):
        return pl.ds(pl.multiple_of(block * ROWS + offset, 16), size)

    def lanes(block):
        return pl.ds(pl.multiple_of(block * ROWS, ROWS), ROWS)

    def remote(src, dst, send, recv, dev):
        return pltpu.make_async_remote_copy(
            src_ref=src, dst_ref=dst, send_sem=send, recv_sem=recv,
            device_id=dev, device_id_type=MESH,
        )

    def a_copy(u, d, recv=0):
        sign = 1 - 2 * d
        block = 2 * zi(-sign * (u // 2 + recv)) + c
        half = u % 2 if d == 0 else 1 - u % 2
        part = X.at[rows(block, HALF * half, HALF)]
        return remote(part, part, a_s.at[d, u], a_r.at[d, u], z_dev(sign))

    def pa_copy(k, recv=0):
        part = X.at[rows(2 * zi(k) + ((1 - c) if recv else c))]
        return remote(part, part, pa_s.at[k], pa_r.at[k], partner)

    def b_block(h, da, db):
        da, db = da % 4, db % 4
        return at(da, db) if h == 0 else at(db, da)

    def b_dev(h, axis, sign):
        along_x = (axis == 0) == (h == 0)
        return x_dev(sign) if along_x else y_dev(sign)

    OFF = (0, -1, 1, 2)

    def b_copy(p, kind, s, h, d, recv=0):
        sign = 1 - 2 * d
        far = 1 if kind in ("first_q", "second_q") else 0
        off, size = (STEP // 2 * d, STEP // 2) if far else (0, STEP)
        if kind in ("first", "first_q"):
            index, block, axis = 2 * far + d, b_block(h, -sign * (far + recv), 0), 0
        else:
            index = 4 + 8 * far + 2 * s + d
            block, axis = b_block(h, OFF[s], -sign * (far + recv)), 1
        part = C.at[rows(block, HALF * p + STEP * h + off, size)]
        return remote(part, part, b_s.at[p, h, index], b_r.at[p, h, index], b_dev(h, axis, sign))

    def d_copy(p, pair, recv=0):
        src = pall.at[rows(2 * pair + (c if recv else (1 - c)), HALF * p, HALF)]
        return remote(src, prx.at[rows(pair, HALF * p, HALF)], d_s.at[p, pair], d_r.at[p, pair], partner)

    def c_copy(p, u, d):
        return remote(sb.at[p, d, u], rb.at[p, d, u], c_s.at[p, d, u], c_r.at[p, d, u], z_dev(1 - 2 * d))

    def fz_copy(u, d, recv=0):
        sign = 1 - 2 * d
        slot = fz.at[zi(-sign * (u + recv))]
        return remote(slot, slot, fz_s.at[d, u], fz_r.at[d, u], z_dev(sign))

    def fx_copy(i, recv=0):
        sign = -1 if i == 1 else 1
        slot = fx.at[lax.rem(x + ((-sign * recv - (i == 2)) % XN), XN)]
        return remote(slot, slot, fx_s.at[i], fx_r.at[i], x_dev(sign))

    def fy_copy(i, recv=0):
        sign = -1 if i == 1 else 1
        slot = fy.at[lax.rem(y + ((-sign * recv - (i == 2)) % YN), YN)]
        return remote(slot, slot, fy_s.at[i], fy_r.at[i], y_dev(sign))

    swap = remote(swap_out, swap_in, fp_s.at[0], fp_r.at[0], partner)

    waited = set()

    def need(name, *key):
        if (name, *key) in waited:
            return
        waited.add((name, *key))
        if name == "a":
            for d in both:
                a_copy(*key, d, 1).wait_recv()
        elif name == "pa":
            pa_copy(*key, 1).wait_recv()
        elif name == "b":
            for h, d in hd:
                b_copy(*key, h, d, 1).wait_recv()
        elif name == "d":
            d_copy(key[0], zi(key[1]), 1).wait_recv()
        elif name == "c":
            for d in both:
                c_copy(*key, d).wait_recv()
        elif name == "fz":
            fz_copy(*key, 1).wait_recv()
        elif name == "fx":
            fx_copy(*key, 1).wait_recv()
        elif name == "fy":
            fy_copy(*key, 1).wait_recv()

    def make_hot(i, carry):
        members = mem_v[pl.ds(i, 1), :]
        ids = lax.broadcasted_iota(jnp.int32, (ROWS, ROWS), 0)
        hit = (lax.rem(ids, 8) == members) & (ids < 24)
        ones = jnp.where(hit, 1.0, 0.0)
        hot[:, lanes(i)] = ones[:16].astype(BF16)
        hot_rows[rows(i)] = ones.T.astype(BF16)
        return carry

    def split(v, out):
        s = v[...]
        hi = s.astype(BF16).astype(F32)
        mid = (s - hi).astype(BF16).astype(F32)
        low = s - hi - mid
        out[...] = jnp.concatenate([hi, mid, low, jnp.zeros_like(s)], axis=0).astype(BF16)

    def stack(parts):
        return parts[0] if len(parts) == 1 else jnp.concatenate(parts, axis=0)

    def scale(parts, size, src, sc, dst):
        ones = stack([hot_rows[part, :32] for part in parts])
        factor = jnp.dot(ones, sc[...], preferred_element_type=F32)
        for i, part in enumerate(parts):
            dst[part] = (src[part].astype(F32) * factor[size * i : size * (i + 1)]).astype(BF16)

    def back(p, *places):
        blocks = [at(dx, dy) for dx, dy in places]
        parts = [rows(block, HALF * p, HALF) for block in blocks]
        scale(parts, HALF, C, sc_out, Cs)
        lhs = stack([Cs[part] for part in parts])
        for n in range(depth // 256):
            cols = pl.ds(256 * n, 256)
            product = jnp.dot(lhs, WT[:, cols], preferred_element_type=F32).astype(BF16)
            for i, part in enumerate(parts):
                pall[part, cols] = product[HALF * i : HALF * (i + 1)]
        for block in blocks:
            @pl.when(lax.rem(block, 2) != c)
            def _():
                d_copy(p, lax.div(block, 2)).start()

    def chip_sum(p, k, half):
        pair, off = zi(k), HALF * p + STEP * half
        own = pall[rows(2 * pair + c, off, STEP)].astype(F32)
        return own + prx[rows(pair, off, STEP)].astype(F32)

    loads = [
        pltpu.make_async_copy(x_hbm, X.at[rows(col)], load_sem.at[0]),
        pltpu.make_async_copy(cot_hbm, C.at[rows(row)], load_sem.at[1]),
        pltpu.make_async_copy(w_hbm, W, load_sem.at[2]),
        pltpu.make_async_copy(sin_hbm, sin_v, load_sem.at[3]),
        pltpu.make_async_copy(sout_hbm, sout_v, load_sem.at[4]),
        pltpu.make_async_copy(mem_hbm, mem_v, load_sem.at[5]),
    ]
    for load in loads:
        load.start()
    barrier = pltpu.get_barrier_semaphore()
    for dev in (z_dev(1), z_dev(-1), x_dev(1), x_dev(-1), y_dev(1), y_dev(-1), partner):
        pl.semaphore_signal(barrier, inc=1, device_id=dev, device_id_type=MESH)
    pl.semaphore_wait(barrier, 7)

    def b_send(p, kind, s=0):
        for h, d in hd:
            b_copy(p, kind, s, h, d).start()

    def b0(p):
        b_send(p, "first")

    def b00(p):
        b_send(p, "second", 0)

    def b1(p):
        need("b", p, "first", 0)
        b_send(p, "first_q")
        b_send(p, "second", 1)
        b_send(p, "second", 2)

    def b2(p):
        need("b", p, "second", 0)
        b_send(p, "second_q", 0)

    def b3(p):
        need("b", p, "first_q", 0)
        b_send(p, "second", 3)

    def b4(p):
        for s in (1, 2):
            need("b", p, "second", s)
            b_send(p, "second_q", s)

    def b5(p):
        need("b", p, "second", 3)
        b_send(p, "second_q", 3)

    def a(u):
        need("a", u)
        if u < 5:
            for d in both:
                a_copy(u + 2, d).start()
        for k in {1: (1, 7), 3: (2, 6), 5: (3, 5), 6: (4,)}.get(u, ()):
            pa_copy(k).start()

    def nbr(p):
        need("b", p, "first", 0)
        need("b", p, "second", 0)
        back(p, (1, 0), (3, 0), (0, 1), (0, 3))

    def diag(p):
        need("b", p, "second", 1)
        need("b", p, "second", 2)
        back(p, (1, 1), (1, 3), (3, 1), (3, 3))

    def anti(p):
        need("b", p, "first_q", 0)
        need("b", p, "second_q", 0)
        back(p, (2, 0), (0, 2))

    def knight(p):
        need("b", p, "second", 3)
        need("b", p, "second_q", 1)
        need("b", p, "second_q", 2)
        back(p, (2, 1), (2, 3), (1, 2), (3, 2))

    def far(p):
        need("b", p, "second_q", 3)
        back(p, (2, 2))

    landed = []

    def pre(k):
        need("pa", k)
        pair = zi(k)
        scale([rows(2 * pair), rows(2 * pair + 1)], ROWS, X, sc_in, Xs)
        two = rows(2 * pair, 0, 2 * ROWS)
        lhs = Xs[two]
        if all(("b", p, "second_q", 3) in waited for p in range(PHASES)):
            landed.append(k)
        for n in range(width // 256):
            cols = pl.ds(256 * n, 256)
            out = jnp.dot(lhs, W[:, cols], preferred_element_type=F32)
            if k in landed:
                out = C[two, cols].astype(F32) * out
            terms[two, cols] = out.astype(BF16)

    def late():
        for k in range(ZN):
            if k not in landed:
                two = rows(2 * zi(k), 0, 2 * ROWS)
                terms[two] = (C[two].astype(F32) * terms[two].astype(F32)).astype(BF16)

    def inx(p):
        def one(i, carry):
            for j in both:
                part = rows(2 * i + j, HALF * p, HALF)
                in_terms[part] = (X[part].astype(F32) * pall[part].astype(F32)).astype(BF16)
            return carry
        for k in range(ZN):
            need("pa", k)
        lax.fori_loop(0, ZN, one, 0)

    def cc(p, u):
        k = 4 - (u + 1) // 2
        for m in (k, -k % ZN):
            need("d", p, m)
        if u >= 2:
            need("c", p, u - 2)
        for d in both:
            half = u % 2 if d == 0 else 1 - u % 2
            total = chip_sum(p, k if d == 0 else -k, half)
            if u >= 2:
                total += rb[p, d, u - 2].astype(F32)
            sb[p, d, u] = total.astype(BF16)
            c_copy(p, u, d).start()

    def fin_rows(p):
        need("d", p, 0)
        need("c", p, 5)
        need("c", p, 6)
        for half in both:
            part = pl.ds(HALF * p + STEP * half, STEP)
            total = chip_sum(p, 0, half)
            total += rb[p, 0, 6 - half].astype(F32) + rb[p, 1, 5 + half].astype(F32)
            ig_v[part] = (total * r_own[part]).astype(BF16)

    def f(i):
        if i == 0:
            partial = jnp.dot(hot[...], in_terms[...], preferred_element_type=F32)
            fz[z] = partial[:8].astype(BF16)
        if 0 < i < 4:
            for d in both:
                need("fz", i - 1, d)
        if i < 4:
            for d in both:
                if i < 3 or d == 0:
                    fz_copy(i, d).start()
        if i == 4:
            need("fz", 3, 0)
            total = fz[0].astype(F32)
            for k in range(1, ZN):
                total += fz[k].astype(F32)
            swap_out[...] = total
            swap.start()
        if i == 5:
            swap.wait_recv()
            fin[...] = swap_out[...] + swap_in[...]

    def o(i):
        if i == 0:
            fx[x] = jnp.dot(hot[...], terms[...], preferred_element_type=F32)[:8]
            fx_copy(0).start()
            fx_copy(1).start()
        if i == 1:
            need("fx", 0)
            fx_copy(2).start()
        if i == 2:
            need("fx", 1)
            need("fx", 2)
            fy[y] = ((fx[0] + fx[1]) + fx[2]) + fx[3]
            fy_copy(0).start()
            fy_copy(1).start()
        if i == 3:
            need("fy", 0)
            fy_copy(2).start()
        if i == 4:
            need("fy", 1)
            need("fy", 2)
            fout[...] = ((fy[0] + fy[1]) + fy[2]) + fy[3]

    def wg(i):
        cols = pl.ds(256 * i, 256)
        for n in range(width // 256):
            wgs[cols, pl.ds(256 * n, 256)] = lax.dot_general(
                Xs[:, cols], Cs[:, pl.ds(256 * n, 256)], TN, preferred_element_type=F32
            )

    def setup():
        for load in loads[2:]:
            load.wait()
        split(sin_v, sc_in)
        split(sout_v, sc_out)
        lax.fori_loop(0, BLOCKS, make_hot, 0)

        def transpose_step(i, carry):
            src = pl.ds(pl.multiple_of(i * 128, 128), 128)
            for k in range(width // 256):
                WT[pl.ds(256 * k, 256), src] = W[src, pl.ds(256 * k, 256)].T
            return carry
        lax.fori_loop(0, depth // 128, transpose_step, 0)
        r_own[...] = jnp.dot(hot_rows[rows(col), :32], sc_in[...], preferred_element_type=F32)
        back(0, (0, 0))
        back(1, (0, 0))

    loads[1].wait()
    b_send(0, "first")
    loads[0].wait()
    for u in (0, 1):
        for d in both:
            a_copy(u, d).start()
    b_send(0, "second", 0)
    pa_copy(0).start()
    setup()
    b0(1)
    b1(0)
    a(0)
    pre(0)
    nbr(0)
    b2(0)
    b3(0)
    a(1)
    b00(1)
    pre(1)
    b4(0)
    a(2)
    diag(0)
    b5(0)
    b1(1)
    anti(0)
    a(3)
    b2(1)
    nbr(1)
    knight(0)
    a(4)
    far(0)
    pre(6)
    b3(1)
    pre(7)
    cc(0, 0)
    a(5)
    b4(1)
    diag(1)
    cc(0, 1)
    anti(1)
    pre(5)
    a(6)
    b5(1)
    pre(2)
    cc(0, 2)
    knight(1)
    inx(0)
    cc(0, 3)
    far(1)
    inx(1)
    f(0)
    cc(1, 0)
    pre(4)
    cc(1, 1)
    cc(0, 4)
    pre(3)
    late()
    o(0)
    f(1)
    cc(1, 2)
    wg(3)
    cc(1, 3)
    o(1)
    cc(0, 5)
    wg(1)
    f(2)
    cc(1, 4)
    wg(0)
    cc(1, 5)
    o(2)
    f(3)
    cc(0, 6)
    cc(1, 6)
    o(3)
    f(4)
    wg(2)
    f(5)
    fin_rows(0)
    o(4)
    fin_rows(1)
    for d in both:
        for u in range(7):
            a_copy(u, d).wait_send()
            for p in range(PHASES):
                c_copy(p, u, d).wait_send()
        for u in range(3):
            fz_copy(u, d).wait_send()
    fz_copy(3, 0).wait_send()
    for k in range(ZN):
        pa_copy(k).wait_send()
        for p in range(PHASES):
            d_copy(p, k).wait_send()
    for p in range(PHASES):
        for h, d in hd:
            for kind in ("first", "first_q"):
                b_copy(p, kind, 0, h, d).wait_send()
            for kind in ("second", "second_q"):
                for s in range(4):
                    b_copy(p, kind, s, h, d).wait_send()
    for u in range(3):
        fx_copy(u).wait_send()
        fy_copy(u).wait_send()
    swap.wait_send()


def write_out(*refs):
    sems = refs[-1]
    ig_v, wg_v, fin_v, fout_v, ig_o, wg_o, fin_o, fout_o = refs[:-1]
    copies = []
    depth = wg_v.shape[0]
    parts = [(ig_v, ig_o), (fin_v, fin_o), (fout_v, fout_o)]
    for i in range(4):
        part = pl.ds(depth // 4 * i, depth // 4)
        parts.append((wg_v.at[part], wg_o.at[part]))
    for i, (src, dst) in enumerate(parts):
        copies.append(pltpu.make_async_copy(src, dst, sems.at[i]))
        copies[-1].start()
    for copy in copies:
        copy.wait()


def local(inputs, weight, cotangent, scale_in, scale_out, member):
    depth, width = weight.shape
    batch = BLOCKS * ROWS
    in_hbm = pl.BlockSpec(memory_space=pltpu.HBM)
    in_vmem = pl.BlockSpec(memory_space=pltpu.VMEM)
    dma = pltpu.SemaphoreType.DMA
    outs = (
        ((ROWS, depth), BF16),
        ((depth, width), F32),
        ((8, depth), F32),
        ((8, width), F32),
    )
    results = pl.pallas_call(
        kernel,
        out_shape=tuple(pltpu.VMEM(*out) for out in outs),
        in_specs=[in_hbm] * 6,
        out_specs=(in_vmem,) * 4,
        scratch_shapes=[
            pltpu.VMEM((batch, depth), BF16),
            pltpu.VMEM((batch, width), BF16),
            pltpu.VMEM((batch, depth), BF16),
            pltpu.VMEM((batch, width), BF16),
            pltpu.VMEM((depth, width), BF16),
            pltpu.VMEM((width, depth), BF16),
            pltpu.VMEM((batch, depth), BF16),
            pltpu.VMEM((batch // 2, depth), BF16),
            pltpu.VMEM((PHASES, 2, 7, STEP, depth), BF16),
            pltpu.VMEM((PHASES, 2, 7, STEP, depth), BF16),
            pltpu.VMEM((ROWS, depth), F32),
            pltpu.VMEM((8, depth), F32),
            pltpu.VMEM((8, width), F32),
            pltpu.VMEM((BLOCKS, ROWS), jnp.int32),
            pltpu.VMEM((32, depth), BF16),
            pltpu.VMEM((32, width), BF16),
            pltpu.VMEM((16, batch), BF16),
            pltpu.VMEM((batch, ROWS), BF16),
            pltpu.VMEM((batch, width), BF16),
            pltpu.VMEM((batch, depth), BF16),
            pltpu.VMEM((8, depth), F32),
            pltpu.VMEM((8, depth), F32),
            pltpu.VMEM((ZN, 8, depth), BF16),
            pltpu.VMEM((XN, 8, width), F32),
            pltpu.VMEM((YN, 8, width), F32),
            dma((6,)),
            dma((2, 7)), dma((2, 7)), dma((8,)), dma((8,)),
            dma((2, 2, 20)), dma((2, 2, 20)), dma((2, 8)), dma((2, 8)),
            dma((2, 2, 7)), dma((2, 2, 7)),
            dma((1,)), dma((1,)), dma((2, 4)), dma((2, 4)),
            dma((3,)), dma((3,)), dma((3,)), dma((3,)),
        ],
        compiler_params=pltpu.CompilerParams(
            collective_id=0, has_side_effects=True, vmem_limit_bytes=62500000
        ),
    )(inputs, weight, cotangent, scale_in, scale_out, member.reshape(BLOCKS, ROWS))
    return pl.pallas_call(
        write_out,
        out_shape=tuple(jax.ShapeDtypeStruct(*out) for out in outs),
        in_specs=[in_vmem] * 4,
        out_specs=(in_hbm,) * 4,
        scratch_shapes=[dma((7,))],
        compiler_params=pltpu.CompilerParams(vmem_limit_bytes=8 * 1024 * 1024),
    )(*results)


def solution(mesh):
    placed = (
        P("col", "row"),
        P("row", "col"),
        P("row", "col"),
        P(None, "row"),
        P(None, "col"),
        P(),
    )
    return jax.shard_map(
        local,
        mesh=mesh,
        in_specs=placed,
        out_specs=(P("col", "row"), P("row", "col"), P(None, "row"), P(None, "col")),
        check_vma=False,
    )
```

```python
import jax
import jax.numpy as jnp
from jax import lax
from jax.experimental import pallas as pl
from jax.experimental.pallas import tpu as pltpu
from jax.sharding import PartitionSpec as P

MESH = pl.DeviceIdType.MESH
BF16 = jnp.bfloat16
F32 = jnp.float32
XN, YN, ZN = 4, 4, 8
ROWS = 128
HALF = 64
PHASES = 2
STEP = 32
BLOCKS = 16
LONG_HOP = {"x": 1, "y": 1, "z": 0}
TN = (((0,), (0,)), ((), ()))


def kernel(
    x_hbm, w_hbm, cot_hbm, sin_hbm, sout_hbm, mem_hbm,
    ig_v, wgs, fin, fout,
    X, C, Xs, Cs, W, WT, pall, prx, sb, rb, r_own,
    sin_v, sout_v, mem_v, sc_in, sc_out,
    hot, hot_rows, terms, in_terms, swap_out, swap_in, fz, fx, fy,
    load_sem,
    a_s, a_r, pa_s, pa_r, b_s, b_r, d_s, d_r, c_s, c_r,
    fp_s, fp_r, fz_s, fz_r, fx_s, fx_r, fy_s, fy_r,
):
    row, col = lax.axis_index("row"), lax.axis_index("col")
    x, y = lax.div(row, YN), lax.rem(row, YN)
    z, c = lax.div(col, 2), lax.rem(col, 2)
    depth, width = W.shape
    both = (0, 1)
    place = {"x": x, "y": y, "z": z}

    def way(axis, q):
        return lax.rem(place[axis] + (q + LONG_HOP[axis]), 2)

    def sign(axis, q):
        return 1 - 2 * way(axis, q)

    def zi(k):
        return lax.rem(z + (k % ZN if isinstance(k, int) else k + ZN), ZN)

    def at(dx, dy):
        dx, dy = (v % 4 if isinstance(v, int) else v + 4 for v in (dx, dy))
        return YN * lax.rem(x + dx, XN) + lax.rem(y + dy, YN)

    def z_dev(k):
        return (row, 2 * zi(k) + c)

    partner = (row, 2 * z + 1 - c)

    def x_dev(k):
        return (at(k, 0), col)

    def y_dev(k):
        return (at(0, k), col)

    def rows(block, offset=0, size=ROWS):
        return pl.ds(pl.multiple_of(block * ROWS + offset, 16), size)

    def lanes(block):
        return pl.ds(pl.multiple_of(block * ROWS, ROWS), ROWS)

    def remote(src, dst, send, recv, dev):
        return pltpu.make_async_remote_copy(
            src_ref=src, dst_ref=dst, send_sem=send, recv_sem=recv,
            device_id=dev, device_id_type=MESH,
        )

    def a_copy(u, q, recv=0):
        d, sg = way("z", q), sign("z", q)
        block = 2 * zi(-sg * (u // 2 + recv)) + c
        half = lax.rem(u + d, 2)
        part = X.at[rows(block, HALF * half, HALF)]
        return remote(part, part, a_s.at[d, u], a_r.at[d, u], z_dev(sg))

    def pa_copy(k, recv=0):
        part = X.at[rows(2 * zi(k) + ((1 - c) if recv else c))]
        slot = zi(k)
        return remote(part, part, pa_s.at[slot], pa_r.at[slot], partner)

    def b_axis(h, axis):
        return "x" if (axis == 0) == (h == 0) else "y"

    def b_block(h, da, db):
        return at(da, db) if h == 0 else at(db, da)

    def b_copy(p, kind, s, h, q, recv=0):
        far = 1 if kind in ("first_q", "second_q") else 0
        name = b_axis(h, 0 if kind in ("first", "first_q") else 1)
        d, sg = way(name, q), sign(name, q)
        off, size = (STEP // 2 * d, STEP // 2) if far else (0, STEP)
        if name == b_axis(h, 0):
            index, block = 2 * far + d, b_block(h, -sg * (far + recv), 0)
        else:
            index = 4 + 8 * far + 2 * s + d
            da = -sign(b_axis(h, 0), s - 1) if s in (1, 2) else (0, 0, 0, 2)[s]
            block = b_block(h, da, -sg * (far + recv))
        part = C.at[rows(block, HALF * p + STEP * h + off, size)]
        dev = x_dev(sg) if name == "x" else y_dev(sg)
        return remote(part, part, b_s.at[p, h, index], b_r.at[p, h, index], dev)

    def d_copy(p, pair, recv=0):
        src = pall.at[rows(2 * pair + (c if recv else (1 - c)), HALF * p, HALF)]
        return remote(src, prx.at[rows(pair, HALF * p, HALF)], d_s.at[p, pair], d_r.at[p, pair], partner)

    def c_copy(p, u, q):
        d = way("z", q)
        return remote(sb.at[p, d, u], rb.at[p, d, u], c_s.at[p, d, u], c_r.at[p, d, u], z_dev(sign("z", q)))

    def fz_copy(u, q, recv=0):
        d, sg = way("z", q), sign("z", q)
        slot = fz.at[zi(-sg * (u + recv))]
        return remote(slot, slot, fz_s.at[d, u], fz_r.at[d, u], z_dev(sg))

    def fx_copy(i, recv=0):
        sign = -1 if i == 1 else 1
        slot = fx.at[lax.rem(x + ((-sign * recv - (i == 2)) % XN), XN)]
        return remote(slot, slot, fx_s.at[i], fx_r.at[i], x_dev(sign))

    def fy_copy(i, recv=0):
        sign = -1 if i == 1 else 1
        slot = fy.at[lax.rem(y + ((-sign * recv - (i == 2)) % YN), YN)]
        return remote(slot, slot, fy_s.at[i], fy_r.at[i], y_dev(sign))

    swap = remote(swap_out, swap_in, fp_s.at[0], fp_r.at[0], partner)

    waited = set()

    def step_of(j, q=None):
        return j if q is None else -sign("z", q) * j

    def need(name, *key):
        if (name, *key) in waited:
            return
        waited.add((name, *key))
        if name == "a":
            a_copy(*key, 1).wait_recv()
        elif name == "pa":
            pa_copy(step_of(*key), 1).wait_recv()
        elif name == "b":
            p, kind, s, q = key
            for h in both:
                b_copy(p, kind, s, h, q, 1).wait_recv()
        elif name == "d":
            d_copy(key[0], zi(step_of(*key[1:])), 1).wait_recv()
        elif name == "c":
            c_copy(*key).wait_recv()
        elif name == "fz":
            fz_copy(*key, 1).wait_recv()
        elif name == "fx":
            fx_copy(*key, 1).wait_recv()
        elif name == "fy":
            fy_copy(*key, 1).wait_recv()

    def make_hot(i, carry):
        members = mem_v[pl.ds(i, 1), :]
        ids = lax.broadcasted_iota(jnp.int32, (ROWS, ROWS), 0)
        hit = (lax.rem(ids, 8) == members) & (ids < 24)
        ones = jnp.where(hit, 1.0, 0.0)
        hot[:, lanes(i)] = ones[:16].astype(BF16)
        hot_rows[rows(i)] = ones.T.astype(BF16)
        return carry

    def split(v, out):
        s = v[...]
        hi = s.astype(BF16).astype(F32)
        mid = (s - hi).astype(BF16).astype(F32)
        low = s - hi - mid
        out[...] = jnp.concatenate([hi, mid, low, jnp.zeros_like(s)], axis=0).astype(BF16)

    def stack(parts):
        return parts[0] if len(parts) == 1 else jnp.concatenate(parts, axis=0)

    def scale(parts, size, src, sc, dst):
        ones = stack([hot_rows[part, :32] for part in parts])
        factor = jnp.dot(ones, sc[...], preferred_element_type=F32)
        for i, part in enumerate(parts):
            dst[part] = (src[part].astype(F32) * factor[size * i : size * (i + 1)]).astype(BF16)

    def back(p, *places):
        blocks = [at(dx, dy) for dx, dy in places]
        parts = [rows(block, HALF * p, HALF) for block in blocks]
        scale(parts, HALF, C, sc_out, Cs)
        lhs = stack([Cs[part] for part in parts])
        for n in range(depth // 256):
            cols = pl.ds(256 * n, 256)
            product = jnp.dot(lhs, WT[:, cols], preferred_element_type=F32).astype(BF16)
            for i, part in enumerate(parts):
                pall[part, cols] = product[HALF * i : HALF * (i + 1)]
        for block in blocks:
            @pl.when(lax.rem(block, 2) != c)
            def _():
                d_copy(p, lax.div(block, 2)).start()

    def chip_sum(p, k, half):
        pair, off = zi(k), HALF * p + STEP * half
        own = pall[rows(2 * pair + c, off, STEP)].astype(F32)
        return own + prx[rows(pair, off, STEP)].astype(F32)

    loads = [
        pltpu.make_async_copy(x_hbm, X.at[rows(col)], load_sem.at[0]),
        pltpu.make_async_copy(cot_hbm, C.at[rows(row)], load_sem.at[1]),
        pltpu.make_async_copy(w_hbm, W, load_sem.at[2]),
        pltpu.make_async_copy(sin_hbm, sin_v, load_sem.at[3]),
        pltpu.make_async_copy(sout_hbm, sout_v, load_sem.at[4]),
        pltpu.make_async_copy(mem_hbm, mem_v, load_sem.at[5]),
    ]
    for load in loads:
        load.start()
    barrier = pltpu.get_barrier_semaphore()
    for dev in (z_dev(1), z_dev(-1), x_dev(1), x_dev(-1), y_dev(1), y_dev(-1), partner):
        pl.semaphore_signal(barrier, inc=1, device_id=dev, device_id_type=MESH)
    pl.semaphore_wait(barrier, 7)

    def b_send(p, kind, s, qs=both):
        for q in qs:
            for h in both:
                b_copy(p, kind, s, h, q).start()

    def b_need(p, kind, s):
        for q in both:
            need("b", p, kind, s, q)

    def b0(p):
        b_send(p, "first", 0)

    def b00(p):
        b_send(p, "second", 0)

    def b1(p, q):
        need("b", p, "first", 0, q)
        b_send(p, "first_q", 0, (q,))
        b_send(p, "second", 1 + q)

    def b2(p, q):
        need("b", p, "second", 0, q)
        b_send(p, "second_q", 0, (q,))

    def b3(p):
        b_need(p, "first_q", 0)
        b_send(p, "second", 3)

    def b4(p, q):
        for s in (1, 2):
            need("b", p, "second", s, q)
            b_send(p, "second_q", s, (q,))

    def b5(p, q):
        need("b", p, "second", 3, q)
        b_send(p, "second_q", 3, (q,))

    def a(u, q):
        need("a", u, q)
        if u < 5:
            a_copy(u + 2, q).start()
        if u % 2:
            pa_copy(-sign("z", q) * (u // 2 + 1)).start()

    def a6():
        need("a", 6, 0)
        need("a", 6, 1)
        pa_copy(4).start()

    def nbr(p):
        b_need(p, "first", 0)
        b_need(p, "second", 0)
        back(p, (1, 0), (3, 0), (0, 1), (0, 3))

    def diag(p):
        b_need(p, "second", 1)
        b_need(p, "second", 2)
        back(p, (1, 1), (1, 3), (3, 1), (3, 3))

    def anti(p):
        b_need(p, "first_q", 0)
        b_need(p, "second_q", 0)
        back(p, (2, 0), (0, 2))

    def knight(p):
        b_need(p, "second", 3)
        b_need(p, "second_q", 1)
        b_need(p, "second_q", 2)
        back(p, (2, 1), (2, 3), (1, 2), (3, 2))

    def far(p):
        b_need(p, "second_q", 3)
        back(p, (2, 2))

    all_pairs = [(0,), (4,)] + [(j, q) for j in (1, 2, 3) for q in both]
    landed = []

    def pre(*key):
        need("pa", *key)
        pair = zi(step_of(*key))
        scale([rows(2 * pair), rows(2 * pair + 1)], ROWS, X, sc_in, Xs)
        two = rows(2 * pair, 0, 2 * ROWS)
        lhs = Xs[two]
        if all(("b", p, "second_q", 3, q) in waited for p in range(PHASES) for q in both):
            landed.append(key)
        for n in range(width // 256):
            cols = pl.ds(256 * n, 256)
            out = jnp.dot(lhs, W[:, cols], preferred_element_type=F32)
            if key in landed:
                out = C[two, cols].astype(F32) * out
            terms[two, cols] = out.astype(BF16)

    def late():
        for key in all_pairs:
            if key not in landed:
                two = rows(2 * zi(step_of(*key)), 0, 2 * ROWS)
                terms[two] = (C[two].astype(F32) * terms[two].astype(F32)).astype(BF16)

    def inx(p):
        def one(i, carry):
            for j in both:
                part = rows(2 * i + j, HALF * p, HALF)
                in_terms[part] = (X[part].astype(F32) * pall[part].astype(F32)).astype(BF16)
            return carry
        for key in all_pairs:
            need("pa", *key)
        lax.fori_loop(0, ZN, one, 0)

    def cc(p, u, q):
        k = 4 - (u + 1) // 2
        need("d", p, *((4,) if k == 4 else (k, 1 - q)))
        if u >= 2:
            need("c", p, u - 2, q)
        d = way("z", q)
        total = chip_sum(p, sign("z", q) * k, lax.rem(u + d, 2))
        if u >= 2:
            total += rb[p, d, u - 2].astype(F32)
        sb[p, d, u] = total.astype(BF16)
        c_copy(p, u, q).start()

    def fin_rows(p):
        need("d", p, 0)
        for u in (5, 6):
            for q in both:
                need("c", p, u, q)
        for half in both:
            part = pl.ds(HALF * p + STEP * half, STEP)
            total = chip_sum(p, 0, half)
            total += rb[p, 0, 6 - half].astype(F32) + rb[p, 1, 5 + half].astype(F32)
            ig_v[part] = (total * r_own[part]).astype(BF16)

    def f(i, *qs):
        if i == 0:
            partial = jnp.dot(hot[...], in_terms[...], preferred_element_type=F32)
            fz[z] = partial[:8].astype(BF16)
            fz_copy(0, 0).start()
            fz_copy(0, 1).start()
        if 0 < i < 4:
            for q in qs or (0,):
                need("fz", i - 1, q)
                fz_copy(i, q).start()
        if i == 4:
            need("fz", 2, 1)
            need("fz", 3, 1)
            total = fz[0].astype(F32)
            for k in range(1, ZN):
                total += fz[k].astype(F32)
            swap_out[...] = total
            swap.start()
        if i == 5:
            swap.wait_recv()
            fin[...] = swap_out[...] + swap_in[...]

    def o(i):
        if i == 0:
            fx[x] = jnp.dot(hot[...], terms[...], preferred_element_type=F32)[:8]
            fx_copy(0).start()
            fx_copy(1).start()
        if i == 1:
            need("fx", 0)
            fx_copy(2).start()
        if i == 2:
            need("fx", 1)
            need("fx", 2)
            fy[y] = ((fx[0] + fx[1]) + fx[2]) + fx[3]
            fy_copy(0).start()
            fy_copy(1).start()
        if i == 3:
            need("fy", 0)
            fy_copy(2).start()
        if i == 4:
            need("fy", 1)
            need("fy", 2)
            fout[...] = ((fy[0] + fy[1]) + fy[2]) + fy[3]

    def wg(i):
        cols = pl.ds(256 * i, 256)
        for n in range(width // 256):
            wgs[cols, pl.ds(256 * n, 256)] = lax.dot_general(
                Xs[:, cols], Cs[:, pl.ds(256 * n, 256)], TN, preferred_element_type=F32
            )

    def setup():
        for load in loads[2:]:
            load.wait()
        split(sin_v, sc_in)
        split(sout_v, sc_out)
        lax.fori_loop(0, BLOCKS, make_hot, 0)

        def transpose_step(i, carry):
            src = pl.ds(pl.multiple_of(i * 128, 128), 128)
            for k in range(width // 256):
                WT[pl.ds(256 * k, 256), src] = W[src, pl.ds(256 * k, 256)].T
            return carry
        lax.fori_loop(0, depth // 128, transpose_step, 0)
        r_own[...] = jnp.dot(hot_rows[rows(col), :32], sc_in[...], preferred_element_type=F32)
        back(0, (0, 0))
        back(1, (0, 0))

    loads[1].wait()
    b_send(0, "first", 0)
    loads[0].wait()
    for u in (0, 1):
        for q in both:
            a_copy(u, q).start()
    b_send(0, "second", 0)
    pa_copy(0).start()
    setup()
    b0(1)
    b1(0, 0)
    b1(0, 1)
    a(0, 0)
    a(0, 1)
    pre(0)
    nbr(0)
    b2(0, 0)
    b2(0, 1)
    b3(0)
    a(1, 0)
    a(1, 1)
    b00(1)
    pre(1, 0)
    b4(0, 0)
    b4(0, 1)
    a(2, 0)
    a(2, 1)
    diag(0)
    b5(0, 0)
    b5(0, 1)
    b1(1, 0)
    b1(1, 1)
    anti(0)
    a(3, 0)
    a(3, 1)
    b2(1, 0)
    b2(1, 1)
    nbr(1)
    knight(0)
    a(4, 0)
    a(4, 1)
    far(0)
    pre(2, 1)
    b3(1)
    pre(1, 1)
    cc(0, 0, 0)
    cc(0, 0, 1)
    a(5, 0)
    a(5, 1)
    b4(1, 0)
    b4(1, 1)
    diag(1)
    cc(0, 1, 0)
    cc(0, 1, 1)
    anti(1)
    pre(3, 1)
    a6()
    b5(1, 0)
    b5(1, 1)
    pre(2, 0)
    cc(0, 2, 0)
    cc(0, 2, 1)
    knight(1)
    inx(0)
    cc(0, 3, 0)
    cc(0, 3, 1)
    far(1)
    inx(1)
    f(0)
    cc(1, 0, 0)
    cc(1, 0, 1)
    pre(4)
    cc(1, 1, 0)
    cc(1, 1, 1)
    cc(0, 4, 0)
    cc(0, 4, 1)
    pre(3, 0)
    late()
    o(0)
    f(1, 0)
    f(1, 1)
    cc(1, 2, 0)
    cc(1, 2, 1)
    wg(3)
    cc(1, 3, 0)
    cc(1, 3, 1)
    o(1)
    cc(0, 5, 0)
    cc(0, 5, 1)
    wg(1)
    f(2, 0)
    f(2, 1)
    cc(1, 4, 0)
    cc(1, 4, 1)
    wg(0)
    cc(1, 5, 0)
    cc(1, 5, 1)
    o(2)
    f(3)
    cc(0, 6, 0)
    cc(0, 6, 1)
    cc(1, 6, 0)
    cc(1, 6, 1)
    o(3)
    f(4)
    wg(2)
    f(5)
    fin_rows(0)
    o(4)
    fin_rows(1)
    for q in both:
        for u in range(7):
            a_copy(u, q).wait_send()
            for p in range(PHASES):
                c_copy(p, u, q).wait_send()
        for u in range(3):
            fz_copy(u, q).wait_send()
    fz_copy(3, 0).wait_send()
    for k in range(ZN):
        pa_copy(k).wait_send()
        for p in range(PHASES):
            d_copy(p, k).wait_send()
    for p in range(PHASES):
        for h in both:
            for q in both:
                for kind in ("first", "first_q"):
                    b_copy(p, kind, 0, h, q).wait_send()
                for kind in ("second", "second_q"):
                    for s in range(4):
                        b_copy(p, kind, s, h, q).wait_send()
    for u in range(3):
        fx_copy(u).wait_send()
        fy_copy(u).wait_send()
    swap.wait_send()


def write_out(*refs):
    sems = refs[-1]
    ig_v, wg_v, fin_v, fout_v, ig_o, wg_o, fin_o, fout_o = refs[:-1]
    copies = []
    depth = wg_v.shape[0]
    parts = [(ig_v, ig_o), (fin_v, fin_o), (fout_v, fout_o)]
    for i in range(4):
        part = pl.ds(depth // 4 * i, depth // 4)
        parts.append((wg_v.at[part], wg_o.at[part]))
    for i, (src, dst) in enumerate(parts):
        copies.append(pltpu.make_async_copy(src, dst, sems.at[i]))
        copies[-1].start()
    for copy in copies:
        copy.wait()


def local(inputs, weight, cotangent, scale_in, scale_out, member):
    depth, width = weight.shape
    batch = BLOCKS * ROWS
    in_hbm = pl.BlockSpec(memory_space=pltpu.HBM)
    in_vmem = pl.BlockSpec(memory_space=pltpu.VMEM)
    dma = pltpu.SemaphoreType.DMA
    outs = (
        ((ROWS, depth), BF16),
        ((depth, width), F32),
        ((8, depth), F32),
        ((8, width), F32),
    )
    results = pl.pallas_call(
        kernel,
        out_shape=tuple(pltpu.VMEM(*out) for out in outs),
        in_specs=[in_hbm] * 6,
        out_specs=(in_vmem,) * 4,
        scratch_shapes=[
            pltpu.VMEM((batch, depth), BF16),
            pltpu.VMEM((batch, width), BF16),
            pltpu.VMEM((batch, depth), BF16),
            pltpu.VMEM((batch, width), BF16),
            pltpu.VMEM((depth, width), BF16),
            pltpu.VMEM((width, depth), BF16),
            pltpu.VMEM((batch, depth), BF16),
            pltpu.VMEM((batch // 2, depth), BF16),
            pltpu.VMEM((PHASES, 2, 7, STEP, depth), BF16),
            pltpu.VMEM((PHASES, 2, 7, STEP, depth), BF16),
            pltpu.VMEM((ROWS, depth), F32),
            pltpu.VMEM((8, depth), F32),
            pltpu.VMEM((8, width), F32),
            pltpu.VMEM((BLOCKS, ROWS), jnp.int32),
            pltpu.VMEM((32, depth), BF16),
            pltpu.VMEM((32, width), BF16),
            pltpu.VMEM((16, batch), BF16),
            pltpu.VMEM((batch, ROWS), BF16),
            pltpu.VMEM((batch, width), BF16),
            pltpu.VMEM((batch, depth), BF16),
            pltpu.VMEM((8, depth), F32),
            pltpu.VMEM((8, depth), F32),
            pltpu.VMEM((ZN, 8, depth), BF16),
            pltpu.VMEM((XN, 8, width), F32),
            pltpu.VMEM((YN, 8, width), F32),
            dma((6,)),
            dma((2, 7)), dma((2, 7)), dma((8,)), dma((8,)),
            dma((2, 2, 20)), dma((2, 2, 20)), dma((2, 8)), dma((2, 8)),
            dma((2, 2, 7)), dma((2, 2, 7)),
            dma((1,)), dma((1,)), dma((2, 4)), dma((2, 4)),
            dma((3,)), dma((3,)), dma((3,)), dma((3,)),
        ],
        compiler_params=pltpu.CompilerParams(
            collective_id=0, has_side_effects=True, vmem_limit_bytes=62500000
        ),
    )(inputs, weight, cotangent, scale_in, scale_out, member.reshape(BLOCKS, ROWS))
    return pl.pallas_call(
        write_out,
        out_shape=tuple(jax.ShapeDtypeStruct(*out) for out in outs),
        in_specs=[in_vmem] * 4,
        out_specs=(in_hbm,) * 4,
        scratch_shapes=[dma((7,))],
        compiler_params=pltpu.CompilerParams(vmem_limit_bytes=8 * 1024 * 1024),
    )(*results)


def solution(mesh):
    placed = (
        P("col", "row"),
        P("row", "col"),
        P("row", "col"),
        P(None, "row"),
        P(None, "col"),
        P(),
    )
    return jax.shard_map(
        local,
        mesh=mesh,
        in_specs=placed,
        out_specs=(P("col", "row"), P("row", "col"), P(None, "row"), P(None, "col")),
        check_vma=False,
    )
```

```python
import jax
import jax.numpy as jnp
from jax import lax
from jax.experimental import pallas as pl
from jax.experimental.pallas import tpu as pltpu
from jax.sharding import PartitionSpec as P

MESH = pl.DeviceIdType.MESH
BF16 = jnp.bfloat16
F32 = jnp.float32
XN, YN, ZN = 4, 4, 8
ROWS = 128
HALF = 64
PHASES = 2
STEP = 32
BLOCKS = 16
LONG_HOP = {"x": 1, "y": 1, "z": 0}
TN = (((0,), (0,)), ((), ()))


def kernel(
    x_hbm, w_hbm, cot_hbm, sin_hbm, sout_hbm, mem_hbm,
    ig_v, wgs, fin, fout,
    X, C, Xs, Cs, W, WT, pall, prx, sb, rb, r_own,
    sin_v, sout_v, mem_v, sc_in, sc_out,
    hot, hot_rows, terms, in_terms, swap_out, swap_in, fz, fx, fy,
    load_sem,
    a_s, a_r, pa_s, pa_r, b_s, b_r, d_s, d_r, c_s, c_r,
    fp_s, fp_r, fz_s, fz_r, fx_s, fx_r, fy_s, fy_r,
):
    row, col = lax.axis_index("row"), lax.axis_index("col")
    x, y = lax.div(row, YN), lax.rem(row, YN)
    z, c = lax.div(col, 2), lax.rem(col, 2)
    depth, width = W.shape
    both = (0, 1)
    place = {"x": x, "y": y, "z": z}

    def way(axis, q):
        return lax.rem(place[axis] + (q + LONG_HOP[axis]), 2)

    def sign(axis, q):
        return 1 - 2 * way(axis, q)

    def zi(k):
        return lax.rem(z + (k % ZN if isinstance(k, int) else k + ZN), ZN)

    def at(dx, dy):
        dx, dy = (v % 4 if isinstance(v, int) else v + 4 for v in (dx, dy))
        return YN * lax.rem(x + dx, XN) + lax.rem(y + dy, YN)

    def z_dev(k):
        return (row, 2 * zi(k) + c)

    partner = (row, 2 * z + 1 - c)

    def x_dev(k):
        return (at(k, 0), col)

    def y_dev(k):
        return (at(0, k), col)

    def rows(block, offset=0, size=ROWS):
        return pl.ds(pl.multiple_of(block * ROWS + offset, 16), size)

    def lanes(block):
        return pl.ds(pl.multiple_of(block * ROWS, ROWS), ROWS)

    def remote(src, dst, send, recv, dev):
        return pltpu.make_async_remote_copy(
            src_ref=src, dst_ref=dst, send_sem=send, recv_sem=recv,
            device_id=dev, device_id_type=MESH,
        )

    def a_copy(u, q, recv=0):
        d, sg = way("z", q), sign("z", q)
        block = 2 * zi(-sg * (u // 2 + recv)) + c
        half = lax.rem(u + d, 2)
        part = X.at[rows(block, HALF * half, HALF)]
        return remote(part, part, a_s.at[d, u], a_r.at[d, u], z_dev(sg))

    def pa_copy(k, recv=0):
        part = X.at[rows(2 * zi(k) + ((1 - c) if recv else c))]
        slot = zi(k)
        return remote(part, part, pa_s.at[slot], pa_r.at[slot], partner)

    def b_axis(h, axis):
        return "x" if (axis == 0) == (h == 0) else "y"

    def b_block(h, da, db):
        return at(da, db) if h == 0 else at(db, da)

    def b_copy(p, kind, s, h, q, recv=0):
        far = 1 if kind in ("first_q", "second_q") else 0
        name = b_axis(h, 0 if kind in ("first", "first_q") else 1)
        d, sg = way(name, q), sign(name, q)
        off, size = (STEP // 2 * d, STEP // 2) if far else (0, STEP)
        if name == b_axis(h, 0):
            index, block = 2 * far + d, b_block(h, -sg * (far + recv), 0)
        else:
            index = 4 + 8 * far + 2 * s + d
            da = -sign(b_axis(h, 0), s - 1) if s in (1, 2) else (0, 0, 0, 2)[s]
            block = b_block(h, da, -sg * (far + recv))
        part = C.at[rows(block, HALF * p + STEP * h + off, size)]
        dev = x_dev(sg) if name == "x" else y_dev(sg)
        return remote(part, part, b_s.at[p, h, index], b_r.at[p, h, index], dev)

    def d_copy(p, pair, recv=0):
        src = pall.at[rows(2 * pair + (c if recv else (1 - c)), HALF * p, HALF)]
        return remote(src, prx.at[rows(pair, HALF * p, HALF)], d_s.at[p, pair], d_r.at[p, pair], partner)

    def c_copy(p, u, q):
        d = way("z", q)
        return remote(sb.at[p, d, u], rb.at[p, d, u], c_s.at[p, d, u], c_r.at[p, d, u], z_dev(sign("z", q)))

    def fz_copy(u, q, recv=0):
        d, sg = way("z", q), sign("z", q)
        slot = fz.at[zi(-sg * (u + recv))]
        return remote(slot, slot, fz_s.at[d, u], fz_r.at[d, u], z_dev(sg))

    def fx_copy(i, recv=0):
        sign = -1 if i == 1 else 1
        slot = fx.at[lax.rem(x + ((-sign * recv - (i == 2)) % XN), XN)]
        return remote(slot, slot, fx_s.at[i], fx_r.at[i], x_dev(sign))

    def fy_copy(i, recv=0):
        sign = -1 if i == 1 else 1
        slot = fy.at[lax.rem(y + ((-sign * recv - (i == 2)) % YN), YN)]
        return remote(slot, slot, fy_s.at[i], fy_r.at[i], y_dev(sign))

    swap = remote(swap_out, swap_in, fp_s.at[0], fp_r.at[0], partner)

    waited = set()

    def step_of(j, q=None):
        return j if q is None else -sign("z", q) * j

    def need(name, *key):
        if (name, *key) in waited:
            return
        waited.add((name, *key))
        if name == "a":
            a_copy(*key, 1).wait_recv()
        elif name == "pa":
            pa_copy(step_of(*key), 1).wait_recv()
        elif name == "b":
            p, kind, s, q = key
            for h in both:
                b_copy(p, kind, s, h, q, 1).wait_recv()
        elif name == "d":
            d_copy(key[0], zi(step_of(*key[1:])), 1).wait_recv()
        elif name == "c":
            c_copy(*key).wait_recv()
        elif name == "fz":
            fz_copy(*key, 1).wait_recv()
        elif name == "fx":
            fx_copy(*key, 1).wait_recv()
        elif name == "fy":
            fy_copy(*key, 1).wait_recv()

    def make_hot(i, carry):
        members = mem_v[pl.ds(i, 1), :]
        ids = lax.broadcasted_iota(jnp.int32, (ROWS, ROWS), 0)
        hit = (lax.rem(ids, 8) == members) & (ids < 24)
        ones = jnp.where(hit, 1.0, 0.0)
        hot[:, lanes(i)] = ones[:16].astype(BF16)
        hot_rows[rows(i)] = ones.T.astype(BF16)
        return carry

    def split(v, out):
        s = v[...]
        hi = s.astype(BF16).astype(F32)
        mid = (s - hi).astype(BF16).astype(F32)
        low = s - hi - mid
        out[...] = jnp.concatenate([hi, mid, low, jnp.zeros_like(s)], axis=0).astype(BF16)

    def stack(parts):
        return parts[0] if len(parts) == 1 else jnp.concatenate(parts, axis=0)

    def scale(parts, size, src, sc, dst):
        ones = stack([hot_rows[part, :32] for part in parts])
        factor = jnp.dot(ones, sc[...], preferred_element_type=F32)
        for i, part in enumerate(parts):
            dst[part] = (src[part].astype(F32) * factor[size * i : size * (i + 1)]).astype(BF16)

    def back(p, *places):
        blocks = [at(dx, dy) for dx, dy in places]
        parts = [rows(block, HALF * p, HALF) for block in blocks]
        scale(parts, HALF, C, sc_out, Cs)
        lhs = stack([Cs[part] for part in parts])
        for n in range(depth // 256):
            cols = pl.ds(256 * n, 256)
            product = jnp.dot(lhs, WT[:, cols], preferred_element_type=F32).astype(BF16)
            for i, part in enumerate(parts):
                pall[part, cols] = product[HALF * i : HALF * (i + 1)]
        for block in blocks:
            @pl.when(lax.rem(block, 2) != c)
            def _():
                d_copy(p, lax.div(block, 2)).start()

    def chip_sum(p, k, half):
        pair, off = zi(k), HALF * p + STEP * half
        own = pall[rows(2 * pair + c, off, STEP)].astype(F32)
        return own + prx[rows(pair, off, STEP)].astype(F32)

    loads = [
        pltpu.make_async_copy(x_hbm, X.at[rows(col)], load_sem.at[0]),
        pltpu.make_async_copy(cot_hbm, C.at[rows(row)], load_sem.at[1]),
        pltpu.make_async_copy(w_hbm, W, load_sem.at[2]),
        pltpu.make_async_copy(sin_hbm, sin_v, load_sem.at[3]),
        pltpu.make_async_copy(sout_hbm, sout_v, load_sem.at[4]),
        pltpu.make_async_copy(mem_hbm, mem_v, load_sem.at[5]),
    ]
    for load in loads:
        load.start()
    barrier = pltpu.get_barrier_semaphore()
    for dev in (z_dev(1), z_dev(-1), x_dev(1), x_dev(-1), y_dev(1), y_dev(-1), partner):
        pl.semaphore_signal(barrier, inc=1, device_id=dev, device_id_type=MESH)
    pl.semaphore_wait(barrier, 7)

    def b_send(p, kind, s, qs=both):
        for q in qs:
            for h in both:
                b_copy(p, kind, s, h, q).start()

    def b_need(p, kind, s):
        for q in both:
            need("b", p, kind, s, q)

    def b0(p):
        b_send(p, "first", 0)

    def b00(p):
        b_send(p, "second", 0)

    def b1(p, q):
        need("b", p, "first", 0, q)
        b_send(p, "first_q", 0, (q,))
        b_send(p, "second", 1 + q)

    def b2(p, q):
        need("b", p, "second", 0, q)
        b_send(p, "second_q", 0, (q,))

    def b3(p):
        b_need(p, "first_q", 0)
        b_send(p, "second", 3)

    def b4(p, q):
        for s in (1, 2):
            need("b", p, "second", s, q)
            b_send(p, "second_q", s, (q,))

    def b5(p, q):
        need("b", p, "second", 3, q)
        b_send(p, "second_q", 3, (q,))

    def a(u, q):
        need("a", u, q)
        if u < 5:
            a_copy(u + 2, q).start()
        if u % 2:
            pa_copy(-sign("z", q) * (u // 2 + 1)).start()

    def a6():
        need("a", 6, 0)
        need("a", 6, 1)
        pa_copy(4).start()

    def nbr(p):
        b_need(p, "first", 0)
        b_need(p, "second", 0)
        back(p, (1, 0), (3, 0), (0, 1), (0, 3))

    def diag(p):
        b_need(p, "second", 1)
        b_need(p, "second", 2)
        back(p, (1, 1), (1, 3), (3, 1), (3, 3))

    def anti(p):
        b_need(p, "first_q", 0)
        b_need(p, "second_q", 0)
        back(p, (2, 0), (0, 2))

    def knight(p):
        b_need(p, "second", 3)
        b_need(p, "second_q", 1)
        b_need(p, "second_q", 2)
        back(p, (2, 1), (2, 3), (1, 2), (3, 2))

    def far(p):
        b_need(p, "second_q", 3)
        back(p, (2, 2))

    all_pairs = [(0,), (4,)] + [(j, q) for j in (1, 2, 3) for q in both]
    landed = []

    def pre(*key):
        need("pa", *key)
        pair = zi(step_of(*key))
        scale([rows(2 * pair), rows(2 * pair + 1)], ROWS, X, sc_in, Xs)
        two = rows(2 * pair, 0, 2 * ROWS)
        lhs = Xs[two]
        if all(("b", p, "second_q", 3, q) in waited for p in range(PHASES) for q in both):
            landed.append(key)
        for n in range(width // 256):
            cols = pl.ds(256 * n, 256)
            out = jnp.dot(lhs, W[:, cols], preferred_element_type=F32)
            if key in landed:
                out = C[two, cols].astype(F32) * out
            terms[two, cols] = out.astype(BF16)

    def late():
        for key in all_pairs:
            if key not in landed:
                two = rows(2 * zi(step_of(*key)), 0, 2 * ROWS)
                terms[two] = (C[two].astype(F32) * terms[two].astype(F32)).astype(BF16)

    def inx(p):
        def one(i, carry):
            for j in both:
                part = rows(2 * i + j, HALF * p, HALF)
                in_terms[part] = (X[part].astype(F32) * pall[part].astype(F32)).astype(BF16)
            return carry
        for key in all_pairs:
            need("pa", *key)
        lax.fori_loop(0, ZN, one, 0)

    def cc(p, u, q):
        k = 4 - (u + 1) // 2
        need("d", p, *((4,) if k == 4 else (k, 1 - q)))
        if u >= 2:
            need("c", p, u - 2, q)
        d = way("z", q)
        total = chip_sum(p, sign("z", q) * k, lax.rem(u + d, 2))
        if u >= 2:
            total += rb[p, d, u - 2].astype(F32)
        sb[p, d, u] = total.astype(BF16)
        c_copy(p, u, q).start()

    def fin_rows(p):
        need("d", p, 0)
        for u in (5, 6):
            for q in both:
                need("c", p, u, q)
        for half in both:
            part = pl.ds(HALF * p + STEP * half, STEP)
            total = chip_sum(p, 0, half)
            total += rb[p, 0, 6 - half].astype(F32) + rb[p, 1, 5 + half].astype(F32)
            ig_v[part] = (total * r_own[part]).astype(BF16)

    def f(i, *qs):
        if i == 0:
            partial = jnp.dot(hot[...], in_terms[...], preferred_element_type=F32)
            fz[z] = partial[:8].astype(BF16)
            fz_copy(0, 0).start()
            fz_copy(0, 1).start()
        if 0 < i < 4:
            for q in qs or (0,):
                need("fz", i - 1, q)
                fz_copy(i, q).start()
        if i == 4:
            need("fz", 2, 1)
            need("fz", 3, 1)
            total = fz[0].astype(F32)
            for k in range(1, ZN):
                total += fz[k].astype(F32)
            swap_out[...] = total
            swap.start()
        if i == 5:
            swap.wait_recv()
            fin[...] = swap_out[...] + swap_in[...]

    def o(i):
        if i == 0:
            fx[x] = jnp.dot(hot[...], terms[...], preferred_element_type=F32)[:8]
            fx_copy(0).start()
            fx_copy(1).start()
        if i == 1:
            need("fx", 0)
            fx_copy(2).start()
        if i == 2:
            need("fx", 1)
            need("fx", 2)
            fy[y] = ((fx[0] + fx[1]) + fx[2]) + fx[3]
            fy_copy(0).start()
            fy_copy(1).start()
        if i == 3:
            need("fy", 0)
            fy_copy(2).start()
        if i == 4:
            need("fy", 1)
            need("fy", 2)
            fout[...] = ((fy[0] + fy[1]) + fy[2]) + fy[3]

    def wg(i):
        cols = pl.ds(256 * i, 256)
        for n in range(width // 256):
            wgs[cols, pl.ds(256 * n, 256)] = lax.dot_general(
                Xs[:, cols], Cs[:, pl.ds(256 * n, 256)], TN, preferred_element_type=F32
            )

    def setup():
        for load in loads[2:]:
            load.wait()
        split(sin_v, sc_in)
        split(sout_v, sc_out)
        lax.fori_loop(0, BLOCKS, make_hot, 0)

        def transpose_step(i, carry):
            src = pl.ds(pl.multiple_of(i * 128, 128), 128)
            for k in range(width // 256):
                WT[pl.ds(256 * k, 256), src] = W[src, pl.ds(256 * k, 256)].T
            return carry
        lax.fori_loop(0, depth // 128, transpose_step, 0)
        r_own[...] = jnp.dot(hot_rows[rows(col), :32], sc_in[...], preferred_element_type=F32)

    loads[1].wait()
    b_send(0, "first", 0)
    loads[0].wait()
    for u in (0, 1):
        for q in both:
            a_copy(u, q).start()
    b_send(0, "second", 0)
    pa_copy(0).start()
    setup()
    b0(1)
    b1(0, 0)
    b1(0, 1)
    a(0, 0)
    a(0, 1)
    back(0, (0, 0))
    back(1, (0, 0))
    pre(0)
    nbr(0)
    b2(0, 0)
    b2(0, 1)
    b3(0)
    a(1, 0)
    a(1, 1)
    b00(1)
    pre(1, 0)
    b4(0, 0)
    b4(0, 1)
    a(2, 0)
    a(2, 1)
    diag(0)
    b5(0, 0)
    b5(0, 1)
    b1(1, 0)
    b1(1, 1)
    anti(0)
    a(3, 0)
    a(3, 1)
    b2(1, 0)
    b2(1, 1)
    nbr(1)
    knight(0)
    a(4, 0)
    a(4, 1)
    far(0)
    pre(2, 1)
    b3(1)
    pre(1, 1)
    cc(0, 0, 0)
    cc(0, 0, 1)
    a(5, 0)
    a(5, 1)
    b4(1, 0)
    b4(1, 1)
    diag(1)
    cc(0, 1, 0)
    cc(0, 1, 1)
    anti(1)
    pre(3, 1)
    a6()
    b5(1, 0)
    b5(1, 1)
    pre(2, 0)
    cc(0, 2, 0)
    cc(0, 2, 1)
    knight(1)
    inx(0)
    cc(0, 3, 0)
    cc(0, 3, 1)
    far(1)
    inx(1)
    f(0)
    cc(1, 0, 0)
    cc(1, 0, 1)
    pre(4)
    cc(1, 1, 0)
    cc(1, 1, 1)
    cc(0, 4, 0)
    cc(0, 4, 1)
    pre(3, 0)
    late()
    o(0)
    f(1, 0)
    f(1, 1)
    cc(1, 2, 0)
    cc(1, 2, 1)
    wg(3)
    cc(1, 3, 0)
    cc(1, 3, 1)
    o(1)
    cc(0, 5, 0)
    cc(0, 5, 1)
    wg(1)
    f(2, 0)
    f(2, 1)
    cc(1, 4, 0)
    cc(1, 4, 1)
    wg(0)
    cc(1, 5, 0)
    cc(1, 5, 1)
    o(2)
    f(3)
    cc(0, 6, 0)
    cc(0, 6, 1)
    cc(1, 6, 0)
    cc(1, 6, 1)
    o(3)
    f(4)
    wg(2)
    f(5)
    fin_rows(0)
    o(4)
    fin_rows(1)
    for q in both:
        for u in range(7):
            a_copy(u, q).wait_send()
            for p in range(PHASES):
                c_copy(p, u, q).wait_send()
        for u in range(3):
            fz_copy(u, q).wait_send()
    fz_copy(3, 0).wait_send()
    for k in range(ZN):
        pa_copy(k).wait_send()
        for p in range(PHASES):
            d_copy(p, k).wait_send()
    for p in range(PHASES):
        for h in both:
            for q in both:
                for kind in ("first", "first_q"):
                    b_copy(p, kind, 0, h, q).wait_send()
                for kind in ("second", "second_q"):
                    for s in range(4):
                        b_copy(p, kind, s, h, q).wait_send()
    for u in range(3):
        fx_copy(u).wait_send()
        fy_copy(u).wait_send()
    swap.wait_send()


def write_out(*refs):
    sems = refs[-1]
    ig_v, wg_v, fin_v, fout_v, ig_o, wg_o, fin_o, fout_o = refs[:-1]
    copies = []
    depth = wg_v.shape[0]
    parts = [(ig_v, ig_o), (fin_v, fin_o), (fout_v, fout_o)]
    for i in range(4):
        part = pl.ds(depth // 4 * i, depth // 4)
        parts.append((wg_v.at[part], wg_o.at[part]))
    for i, (src, dst) in enumerate(parts):
        copies.append(pltpu.make_async_copy(src, dst, sems.at[i]))
        copies[-1].start()
    for copy in copies:
        copy.wait()


def local(inputs, weight, cotangent, scale_in, scale_out, member):
    depth, width = weight.shape
    batch = BLOCKS * ROWS
    in_hbm = pl.BlockSpec(memory_space=pltpu.HBM)
    in_vmem = pl.BlockSpec(memory_space=pltpu.VMEM)
    dma = pltpu.SemaphoreType.DMA
    outs = (
        ((ROWS, depth), BF16),
        ((depth, width), F32),
        ((8, depth), F32),
        ((8, width), F32),
    )
    results = pl.pallas_call(
        kernel,
        out_shape=tuple(pltpu.VMEM(*out) for out in outs),
        in_specs=[in_hbm] * 6,
        out_specs=(in_vmem,) * 4,
        scratch_shapes=[
            pltpu.VMEM((batch, depth), BF16),
            pltpu.VMEM((batch, width), BF16),
            pltpu.VMEM((batch, depth), BF16),
            pltpu.VMEM((batch, width), BF16),
            pltpu.VMEM((depth, width), BF16),
            pltpu.VMEM((width, depth), BF16),
            pltpu.VMEM((batch, depth), BF16),
            pltpu.VMEM((batch // 2, depth), BF16),
            pltpu.VMEM((PHASES, 2, 7, STEP, depth), BF16),
            pltpu.VMEM((PHASES, 2, 7, STEP, depth), BF16),
            pltpu.VMEM((ROWS, depth), F32),
            pltpu.VMEM((8, depth), F32),
            pltpu.VMEM((8, width), F32),
            pltpu.VMEM((BLOCKS, ROWS), jnp.int32),
            pltpu.VMEM((32, depth), BF16),
            pltpu.VMEM((32, width), BF16),
            pltpu.VMEM((16, batch), BF16),
            pltpu.VMEM((batch, ROWS), BF16),
            pltpu.VMEM((batch, width), BF16),
            pltpu.VMEM((batch, depth), BF16),
            pltpu.VMEM((8, depth), F32),
            pltpu.VMEM((8, depth), F32),
            pltpu.VMEM((ZN, 8, depth), BF16),
            pltpu.VMEM((XN, 8, width), F32),
            pltpu.VMEM((YN, 8, width), F32),
            dma((6,)),
            dma((2, 7)), dma((2, 7)), dma((8,)), dma((8,)),
            dma((2, 2, 20)), dma((2, 2, 20)), dma((2, 8)), dma((2, 8)),
            dma((2, 2, 7)), dma((2, 2, 7)),
            dma((1,)), dma((1,)), dma((2, 4)), dma((2, 4)),
            dma((3,)), dma((3,)), dma((3,)), dma((3,)),
        ],
        compiler_params=pltpu.CompilerParams(
            collective_id=0, has_side_effects=True, vmem_limit_bytes=62500000
        ),
    )(inputs, weight, cotangent, scale_in, scale_out, member.reshape(BLOCKS, ROWS))
    return pl.pallas_call(
        write_out,
        out_shape=tuple(jax.ShapeDtypeStruct(*out) for out in outs),
        in_specs=[in_vmem] * 4,
        out_specs=(in_hbm,) * 4,
        scratch_shapes=[dma((7,))],
        compiler_params=pltpu.CompilerParams(vmem_limit_bytes=8 * 1024 * 1024),
    )(*results)


def solution(mesh):
    placed = (
        P("col", "row"),
        P("row", "col"),
        P("row", "col"),
        P(None, "row"),
        P(None, "col"),
        P(),
    )
    return jax.shard_map(
        local,
        mesh=mesh,
        in_specs=placed,
        out_specs=(P("col", "row"), P("row", "col"), P(None, "row"), P(None, "col")),
        check_vma=False,
    )
```
